32 devices in a mesh: rows: 8 (over z, x), leaf: 4 (over y, core).
Axes of the slice: x: 2, y: 2, z: 4, core: 2. Of those that a mesh axis runs over, the one named last changes fastest.
Arguments:
- right_sides: float32 [65536, 128], P(('rows', 'leaf')), may hold values from -30 to 30
- near_blocks: bfloat16 [2, 128, 512, 512], P(None, ('rows', 'leaf')), may hold values from -1 to 2.4
- leaf_bases: bfloat16 [2, 128, 2, 512, 128], P(None, ('rows', 'leaf')), may hold values from -1.5 to 1.5
- local_factors: bfloat16 [2, 224, 3, 128, 128], P(None, ('rows', 'leaf')), may hold values from -1.7 to 1.7
- upper_factors: bfloat16 [2, 32, 3, 3, 128, 128], P(None, ('rows', 'leaf')), may hold values from -1.7 to 1.7, as said below
- top_couplings: bfloat16 [2, 2, 128, 128], replicated, may hold values from -0.5 to 0.5
Outputs:
- solution: float32 [65536, 128], P(('rows', 'leaf'))
- residual_norms: float32 [3, 128], replicated
The draws below stay inside these ranges and needn't reach their ends.
Inputs may be any that keep to these rules, and one draw needn't show every extreme that they name: upper_factors[s, d, h] is the same for all devices d with the same d // 2 ** (h + 1): the factors of the node h + 1 levels above device d's own node.
All inputs are finite; a program needn't handle non-finite values.
Results may differ from the reference program's by a relative error of at most 0.00095.
Values sent between devices are 32-bit elements; how exact they have to be, the bound alone decides.
A program may use at most 128 MiB of HBM per device.

```python
import math
import jax
import jax.numpy as jnp
from jax import lax

LEAF = 512
RANK = 128
RHS = 128
LEAF_DEV = 4
STEPS = 3
UPPER = 3
NLEAVES = 128
ORDER = 65536
N_ROWS = 8
N_LEAF = 4


def clipped(key_value, shape):
    return jnp.clip(jax.random.normal(key_value, shape, jnp.float32), -6.0, 6.0)


def node_factors(key_value, node_count):
    keys = jax.random.split(key_value, 6)
    shape = (node_count, RANK, RANK)
    spread = RANK ** (-0.5)
    identity_matrix = jnp.eye(RANK, dtype=jnp.float32)
    up_transfer = (identity_matrix + 0.3 * spread * clipped(keys[0], shape)) * 0.7071
    down_transfer = (identity_matrix + 0.3 * spread * clipped(keys[1], shape)) * 0.96
    coupling = 0.1 * spread * clipped(keys[2], shape)
    operator_part = jnp.stack([up_transfer, down_transfer, coupling], axis=1)
    inverse_part = jnp.stack([up_transfer + 0.05 * spread * clipped(keys[3], shape), down_transfer + 0.05 * spread * clipped(keys[4], shape), 0.02 * spread * clipped(keys[5], shape) - coupling], axis=1)
    return (operator_part, inverse_part)


def draw_right_sides(key, part):
    first_key = jax.random.fold_in(jax.random.fold_in(key, 606), 0)
    growth = jnp.exp(math.log(3.0) * jnp.arange(ORDER, dtype=jnp.float32) / ORDER)
    return clipped(first_key, (ORDER, RHS)) * growth[:, None]


def draw_near_blocks(key, part):
    keys = jax.random.split(jax.random.fold_in(key, 404), 3)
    diagonal_gain = jax.random.uniform(keys[0], (NLEAVES, LEAF), jnp.float32, 0.8, 1.25)
    coupling = clipped(keys[1], (NLEAVES, LEAF, LEAF)) * (0.2 * LEAF ** (-0.5))
    noise_term = clipped(keys[2], (NLEAVES, LEAF, LEAF)) * (0.45 * LEAF ** (-0.5))
    identity_matrix = jnp.eye(LEAF, dtype=jnp.float32)
    operator_block = identity_matrix * diagonal_gain[:, :, None] + coupling
    inverse_gain = 1.0 / diagonal_gain
    inverse_block = identity_matrix * inverse_gain[:, :, None] - inverse_gain[:, :, None] * coupling * inverse_gain[:, None, :] + noise_term
    return jnp.stack([operator_block, inverse_block]).astype(jnp.bfloat16)


def draw_leaf_bases(key, part):
    first_key, second_key = jax.random.split(jax.random.fold_in(key, 505))
    shape = (NLEAVES, 2, LEAF, RANK)
    operator_bases = clipped(first_key, shape) * LEAF ** (-0.5)
    inverse_bases = operator_bases + 0.1 * clipped(second_key, shape) * LEAF ** (-0.5)
    return jnp.stack([operator_bases, inverse_bases]).astype(jnp.bfloat16)


def draw_local_factors(key, part):
    operator_part, inverse_part = node_factors(jax.random.fold_in(key, 101), (2 * LEAF_DEV - 1) * N_ROWS * N_LEAF)
    return jnp.stack([operator_part, inverse_part]).astype(jnp.bfloat16)


def draw_upper_factors(key, part):
    operator_levels = []
    inverse_levels = []
    for height in range(1, UPPER + 1):
        node_count = N_ROWS * N_LEAF // 2 ** height
        operator_part, inverse_part = node_factors(jax.random.fold_in(jax.random.fold_in(key, 202), height), node_count)
        operator_levels.append(jnp.repeat(operator_part, 2 ** height, axis=0))
        inverse_levels.append(jnp.repeat(inverse_part, 2 ** height, axis=0))
    return jnp.stack([jnp.stack(operator_levels, axis=1), jnp.stack(inverse_levels, axis=1)]).astype(jnp.bfloat16)


def draw_top_couplings(key, part):
    first_key, second_key = jax.random.split(jax.random.fold_in(key, 303))
    spread = RANK ** (-0.5)
    coupling = 0.1 * spread * clipped(first_key, (2, RANK, RANK))
    inverse_coupling = 0.02 * spread * clipped(second_key, (2, RANK, RANK)) - coupling
    return jnp.stack([coupling, inverse_coupling]).astype(jnp.bfloat16)


def setup_inputs(seed: int = 0) -> dict:
    seeds = jax.random.split(jax.random.key(seed), 7)
    return {
        "right_sides": draw_right_sides(jax.random.fold_in(seeds[6], 71), 0),
        "near_blocks": draw_near_blocks(jax.random.fold_in(seeds[6], 71), 0),
        "leaf_bases": draw_leaf_bases(jax.random.fold_in(seeds[6], 71), 0),
        "local_factors": draw_local_factors(jax.random.fold_in(seeds[6], 71), 0),
        "upper_factors": draw_upper_factors(jax.random.fold_in(seeds[6], 71), 0),
        "top_couplings": draw_top_couplings(jax.random.fold_in(seeds[6], 71), 0),
    }


HIGHEST = lax.Precision.HIGHEST


def split_pair(values):
    upper_half = lax.optimization_barrier(values.astype(jnp.bfloat16))
    lower_half = (values - upper_half.astype(jnp.float32)).astype(jnp.bfloat16)
    return (upper_half, lower_half)


def sibling_of(values):
    shaped = values.reshape((values.shape[0] // 2, 2) + values.shape[1:])
    return shaped[:, ::-1].reshape(values.shape)


def level_tables(local_factors, upper_factors, member):
    per_device = local_factors[member].reshape(N_ROWS * N_LEAF, 2 * LEAF_DEV - 1, 3, RANK, RANK)
    tables = []
    offset = 0
    node_count = LEAF_DEV
    while node_count >= 1:
        factor_block = per_device[:, offset:offset + node_count]
        tables.append(factor_block.reshape(-1, 3, RANK, RANK).astype(jnp.float32))
        offset = offset + node_count
        node_count = node_count // 2
    for height in range(1, UPPER + 1):
        tables.append(upper_factors[member, ::2 ** height, height - 1].astype(jnp.float32))
    return tables


def near_and_coefficient(items):
    square, column_basis, stacked_pieces = items
    near_field = jnp.zeros((square.shape[0], stacked_pieces.shape[2]), jnp.float32)
    coefficient = jnp.zeros((column_basis.shape[1], stacked_pieces.shape[2]), jnp.float32)
    for piece_index in range(stacked_pieces.shape[0]):
        piece_value = stacked_pieces[piece_index]
        near_field = near_field + jnp.dot(square, piece_value, preferred_element_type=jnp.float32)
        coefficient = coefficient + jnp.dot(column_basis.T, piece_value, preferred_element_type=jnp.float32)
    return near_field, coefficient


def far_product(items):
    row_basis, stacked_far = items
    result = jnp.zeros((row_basis.shape[0], stacked_far.shape[2]), jnp.float32)
    for piece_index in range(stacked_far.shape[0]):
        result = result + jnp.dot(row_basis, stacked_far[piece_index], preferred_element_type=jnp.float32)
    return result


def apply_tree(near_set, basis_set, tables, top_pair, pieces, split_far):
    stacked = jnp.stack(pieces, axis=1)
    near_field, coefficient = lax.map(near_and_coefficient, (near_set, basis_set[:, 1], stacked))
    lower_list = []
    for factor_table in tables:
        lower_list.append(coefficient)
        projected = jnp.einsum("nab,nac->nbc", factor_table[:, 0], coefficient, precision=HIGHEST)
        coefficient = projected[0::2] + projected[1::2]
    far_field = jnp.einsum("nab,nbc->nac", top_pair.astype(jnp.float32), sibling_of(coefficient), precision=HIGHEST)
    for factor_table, lower_value in zip(tables[::-1], lower_list[::-1]):
        far_field = jnp.einsum("nab,nbc->nac", factor_table[:, 1], jnp.repeat(far_field, 2, axis=0), precision=HIGHEST) + jnp.einsum("nab,nbc->nac", factor_table[:, 2], sibling_of(lower_value), precision=HIGHEST)
    if split_far:
        far_parts = split_pair(far_field)
    else:
        far_parts = (far_field.astype(jnp.bfloat16),)
    return near_field + lax.map(far_product, (basis_set[:, 0], jnp.stack(far_parts, axis=1)))


def reference(right_sides, near_blocks, leaf_bases, local_factors, upper_factors, top_couplings):
    leaves = right_sides.shape[0] // LEAF
    right_side = right_sides.reshape(leaves, LEAF, RHS)
    tables_operator = level_tables(local_factors, upper_factors, 0)
    tables_inverse = level_tables(local_factors, upper_factors, 1)

    def operator(values):
        return apply_tree(near_blocks[0], leaf_bases[0], tables_operator, top_couplings[0], split_pair(values), True)

    def inverse(values):
        return apply_tree(near_blocks[1], leaf_bases[1], tables_inverse, top_couplings[1], (values.astype(jnp.bfloat16),), False)

    solution = inverse(right_side)
    norm_list = []
    for refine_step in range(STEPS):
        residual = right_side - operator(solution)
        norm_list.append(jnp.sum(residual * residual, axis=(0, 1)))
        solution = solution + inverse(residual)
    return (solution.reshape(right_sides.shape[0], RHS), jnp.stack(norm_list))
```

```python
import functools
import jax
import jax.numpy as jnp
from jax import lax
from jax.experimental import pallas as pl
from jax.experimental.pallas import tpu as pltpu
from jax.sharding import PartitionSpec as P

STEPS = 3
F32 = jnp.float32
BF16 = jnp.bfloat16
NT = (((1,), (1,)), ((), ()))


def dot(a, b):
    return jnp.dot(a, b, preferred_element_type=F32)


def split(v):
    hi = v.astype(BF16)
    lo = (v - hi.astype(F32)).astype(BF16)
    return hi, lo


def wide(v):
    return jnp.concatenate(split(v), axis=1)


def tall(v):
    return jnp.concatenate(split(v), axis=0)


def fold_cols(v):
    n = v.shape[1] // 2
    return v[:, :n] + v[:, n:]


def fold_rows(v):
    n = v.shape[0] // 2
    return v[:n] + v[n:]


def combine(out):
    n, m = out.shape[0] // 2, out.shape[1] // 2
    return out[:n, :m] + (out[:n, m:] + out[n:, :m])


def mm(a, b):
    return combine(dot(tall(a), wide(b)))


def dot_nt(a, b):
    return lax.dot_general(a, b, NT, preferred_element_type=F32)


def rows_of(parts):
    return jnp.concatenate(parts, axis=0)


def lanes_of(parts):
    return jnp.concatenate(parts, axis=1)


def norm_rounds(levels):
    return [(lo, min(lo + 5, levels)) for lo in range(0, levels, 5)]


def group_bits(levels):
    return min(3, levels - 2)


def kernel(
    bits_leaf, bits_rows,
    rhs_hbm, near_hbm, bases_hbm, local_hbm, upper_hbm, top_hbm,
    x_ref, norm_ref,
    b_ref, r_ref, near, bases, local, upper, top,
    vt, pt, tt, et, jt, cb, pre, nrm,
    w_send, w_recv, high_a, got_a, plane,
    send_a, send_b, recv_a, recv_b, sib_full, full,
    fac_send, fac_recv, resp_send, resp_recv,
    up_mat, down_mat, side_mat,
    chains, near_coef, rhs_coef, tree, stack,
    out_a, out_b, in_a, in_b, lift, cross, enter,
    fall_a, fall_b, leaf_a, leaf_b, xw, rb, field_a, field_b,
    jw_send, jw_recv, jhigh, jgot, jplane,
    js_a, js_b, jr_a, jr_b, jsib, jfull,
    nsend, nrecv,
    load_sem, send_sem, recv_sem, jsend_sem, jrecv_sem, fsend_sem, frecv_sem, nsend_sem, nrecv_sem,
):
    leaves = near.shape[1]
    levels = bits_leaf + bits_rows
    last = levels - 1
    bits = group_bits(levels)
    group = 2**bits
    root = 2 * leaves - 2
    leaf = lax.axis_index("leaf")
    rows = lax.axis_index("rows")
    columns = x_ref.shape[2]
    rank = plane.shape[1]
    half = columns // 2
    cut = columns // group
    mine = pl.multiple_of(leaf % 2 * half, half)
    other = pl.multiple_of((1 - leaf % 2) * half, half)
    top_pos = rows // 2 ** (bits_rows - 1)

    def flipped(value, mask):
        for bit in range(mask.bit_length()):
            d = 2**bit
            if mask & d:
                value = value + d - 2 * d * (value // d % 2)
        return value

    def device(mask):
        leaf_mask = mask % 2**bits_leaf
        return (flipped(rows, mask // 2**bits_leaf), flipped(leaf, leaf_mask))

    def member(place):
        row, column = place
        if bits <= bits_leaf:
            return column % group
        return column + 2**bits_leaf * (row % 2 ** (bits - bits_leaf))

    me = member((rows, leaf))
    my_rows = pl.multiple_of(me * cut, cut)

    def load(src, dst, index):
        return pltpu.make_async_copy(src, dst, load_sem.at[index])

    loads = {}
    order = []
    for s in (1, 0):
        order += [
            (("local", s), local_hbm.at[s], local.at[s]),
            (("upper", s), upper_hbm.at[s, 0], upper.at[s]),
            (("bases", s), bases_hbm.at[s], bases.at[s]),
        ]
        if s == 1:
            order += [("res", rhs_hbm, r_ref)]
        order += [
            (("near", s), near_hbm.at[s], near.at[s]),
            (("top", s), top_hbm.at[s], top.at[s]),
        ]
        if s == 1:
            order += [("rhs", rhs_hbm, b_ref)]
    for index, (name, src, dst) in enumerate(order):
        loads[name] = load(src, dst, index)
        loads[name].start()

    barrier = pltpu.get_barrier_semaphore()
    partners = set(range(1, group)) | {2**level for level in range(levels)}
    partners.add(2**last + 2 ** (last - 1))
    for lo, hi in norm_rounds(levels):
        partners |= {m << lo for m in range(1, 2 ** (hi - lo))}
    partners = sorted(partners)
    for mask in partners:
        pl.semaphore_signal(
            barrier, inc=1, device_id=device(mask), device_id_type=pl.DeviceIdType.MESH
        )

    def remote(src, dst, sends, recvs, index, mask, started):
        copy = pltpu.make_async_remote_copy(
            src_ref=src,
            dst_ref=dst,
            send_sem=sends.at[index],
            recv_sem=recvs.at[index],
            device_id=device(mask),
            device_id_type=pl.DeviceIdType.MESH,
        )
        copy.start()
        started.append(copy)
        return copy

    def block(i, n=1):
        return pl.ds(i * rank, n * rank)

    def factor(s, level, which):
        return local[s, root, which] if level == 0 else upper[s, level - 1, which]


    def chain(s, which):
        product = upper[s, bits - 2, which].astype(F32)
        for index in range(bits - 3, -1, -1):
            product = fold_cols(dot(upper[s, index, which], wide(product)))
        node = {root: fold_cols(dot(local[s, root, which], wide(product)))}
        for n in range(root - 1, -1, -1):
            parent = leaves + n // 2
            node[n] = fold_cols(dot(local[s, n, which], wide(node[parent])))
        return [node[i] for i in range(leaves)]

    def setup_chain(s):
        loads["local", s].wait()
        loads["upper", s].wait()
        et[...] = tall(lanes_of([v.T for v in chain(s, 0)]))

    def setup_up(s):
        loads["bases", s].wait()
        for i in range(leaves):
            vt[s, i] = bases[s, i, 1].astype(F32).T.astype(BF16)

    def setup_pairs(s):
        for p in range(leaves - 1):
            pair = [local[s, 2 * p + j, 0].astype(F32).T.astype(BF16) for j in range(2)]
            pt[p] = lanes_of(pair)

    def setup_couplings(s):
        loads["top", s].wait()
        for first, stop in ((1, bits), (bits, levels)):
            product = None
            for level in range(first, stop):
                coupling = top[s, top_pos] if level == last else upper[s, level - 1, 2]
                if product is None:
                    value = coupling.astype(F32)
                else:
                    value = fold_rows(dot(tall(product), coupling))
                tt[level] = wide(value.T)
                if level + 1 < stop:
                    q = upper[s, level - 1, 1]
                    product = q.astype(F32) if product is None else fold_rows(dot(tall(product), q))

    def setup_down(s):
        jt[...] = tall(rows_of(chain(s, 1)))

    def apply_first(hooks):
        s = 1
        started = []
        hooks = list(hooks)

        def start(src, dst, mask):
            return remote(src, dst, send_sem, recv_sem, len(started), mask, started)

        def across(value, level):
            return combine(dot(tall(value), tt[level]))

        def near_leaf(i):
            x_ref[i] = dot(near[s, i], r_ref[i].astype(BF16))

        def couple(n):
            sibling = n + 1 - 2 * (n % 2)
            pre[n] = fold_cols(dot(local[s, n, 2], cb[sibling]))

        field = {}

        def inner():
            for p in range(leaves - 1):
                stacked = rows_of([cb[2 * p], cb[2 * p + 1]])
                coefficient = fold_cols(dot(pt[p], stacked))
                if p < leaves - 2:
                    cb[leaves + p] = wide(coefficient)
            full[...] = fold_rows(dot(tall(coefficient.T), local[s, root, 0]))
            sib_full[0] = coefficient
            copy_a = start(full.at[pl.ds(other, half)], recv_a.at[0], 1)
            copies_b = [start(sib_full.at[0], sib_full.at[1], 1)]
            yield
            for level in range(1, bits):
                copy_a.wait_recv()
                if level == 1:
                    value = full[pl.ds(mine, half)] + recv_a[0]
                else:
                    value = send_a[level - 1] + recv_a[level - 1]
                if level < bits - 1:
                    send_a[level] = fold_rows(dot(tall(value), upper[s, level - 1, 0]))
                    copy_a = start(send_a.at[level], recv_a.at[level], 2**level)
                send_b[level] = value
                copies_b.append(start(send_b.at[level], recv_b.at[level], 2**level))
                if level == 1:
                    for n in range(root):
                        couple(n)
                    copies_b[0].wait_recv()
                    root_pre = fold_cols(dot(local[s, root, 2], wide(sib_full[1])))
                yield
            far = None
            for level in range(1, bits):
                copies_b[level].wait_recv()
                term = across(recv_b[level], level)
                far = term if far is None else far + term
            sib_full[2, pl.ds(mine, half)] = far
            piece = sib_full.at[2, pl.ds(mine, half)]
            copy = start(piece, piece, 1)
            yield
            copy.wait_recv()
            product = dot_nt(local[s, root, 1], tall(sib_full[2]))
            field[root] = fold_cols(product) + root_pre
            for n in range(root - 1, -1, -1):
                parent = leaves + n // 2
                field[n] = fold_cols(dot(local[s, n, 1], wide(field[parent]))) + pre[n]
            yield

        for i in range(leaves):
            cb[i] = wide(dot(vt[s, i], r_ref[i].astype(BF16)))
        stacked = rows_of([cb[i] for i in range(leaves)])
        outer_t = combine(dot(et[...], stacked)).T
        for j in range(group):
            w_send[j] = outer_t[j * cut : (j + 1) * cut]
        copies_w = []
        for e in range(group - 1, 0, -1):
            copies_w.append(start(w_send.at[member(device(e))], w_recv.at[e], e))
        steps = inner()
        work = list(range(leaves))

        def fill(everything=False):
            if hooks:
                hooks.pop(0)()
            next(steps, None)
            while work:
                near_leaf(work.pop(0))
                if not everything:
                    break

        fill()
        fill()
        for copy in copies_w:
            copy.wait_recv()
        value = w_send[me]
        for e in range(1, group):
            value = value + w_recv[e]
        far = None
        for level in range(bits, last - 1):
            high_a[level] = fold_rows(dot(tall(value), upper[s, level - 1, 0]))
            high_a[levels + level] = value
            copy_a = start(high_a.at[level], got_a.at[level], 2**level)
            copy_b = start(high_a.at[levels + level], got_a.at[levels + 1 + level], 2**level)
            fill()
            copy_a.wait_recv()
            value = high_a[level] + got_a[level]
            copy_b.wait_recv()
            term = across(got_a[levels + 1 + level], level)
            far = term if far is None else far + term
        low, high = last - 1, last
        high_a[high] = fold_rows(dot(tall(value), upper[s, low - 1, 0]))
        high_a[low] = value
        copies_top = [
            start(high_a.at[src], got_a.at[dst], mask)
            for src, dst, mask in (
                (high, high + 1, 2**high + 2**low),
                (high, high, 2**high),
                (low, low, 2**low),
            )
        ]
        fill()
        copies_top[2].wait_recv()
        term = across(got_a[low], low)
        far = term if far is None else far + term
        fill(True)
        copies_top[1].wait_recv()
        copies_top[0].wait_recv()
        far = far + across(got_a[high] + got_a[high + 1], high)
        plane[pl.ds(my_rows, cut)] = far
        copies_f = []
        for e in range(group - 1, 0, -1):
            piece = plane.at[pl.ds(my_rows, cut)]
            copies_f.append(start(piece, piece, e))
        for _ in steps:
            pass
        while hooks:
            hooks.pop(0)()
        for copy in copies_f:
            copy.wait_recv()
        outer = combine(dot_nt(jt[...], tall(plane[...])))
        for i in range(leaves):
            total = field[i] + outer[i * rank : (i + 1) * rank]
            value = x_ref[i] + dot(bases[s, i, 0], total.astype(BF16))
            x_ref[i] = value
            xw[i] = wide(value)
        for copy in started:
            copy.wait_send()


    pending = []
    replies = {}

    def local_chain(s, which):
        node = {}
        for n in range(root - 1, -1, -1):
            parent = leaves + n // 2
            own = local[s, n, which]
            if parent == root:
                node[n] = own.astype(F32)
            else:
                node[n] = fold_cols(dot(own, wide(node[parent])))
        return rows_of([node[i] for i in range(leaves)])

    def product_vu(i):
        return dot(vt[1, i], bases[0, i, 0])

    def send_response(level, value):
        resp_send[level] = value
        replies["response", level] = remote(
            resp_send.at[level], resp_recv.at[level], fsend_sem, frecv_sem,
            levels + level, 2**level, pending,
        )

    def setup_response():
        loads["local", 0].wait()
        loads["upper", 0].wait()
        for level in range(last):
            fac_send[level] = lanes_of(
                [
                    factor(1, level, 0).astype(F32).T,
                    factor(0, level, 1).astype(F32),
                    factor(0, level, 2).astype(F32),
                ]
            )
            replies["factor", level] = remote(
                fac_send.at[level], fac_recv.at[level], fsend_sem, frecv_sem,
                level, 2**level, pending,
            )
        setup_up(0)
        for s in range(2):
            for which in range(2):
                chains[s, which] = local_chain(s, which)
        middle = rows_of([mm(product_vu(i), chains[0, 1, block(i)]) for i in range(leaves)])
        send_response(0, -mm(chains[1, 0].T, middle))

    def pack(level, x, y, d, c0, c1):
        zero = jnp.zeros((rank, rank), F32)
        if x is not None:
            p = [factor(s, level, 0).astype(F32) for s in range(2)]
            q = [factor(s, level, 1).astype(F32).T for s in range(2)]
            up_mat[level] = rows_of([lanes_of([p[0], x.T]), lanes_of([zero, p[1]])])
            down_mat[level] = rows_of([lanes_of([q[0], y.T]), lanes_of([zero, q[1]])])
            lift[level] = wide(up_mat[level])
        side_mat[level] = rows_of(
            [lanes_of([c0.astype(F32).T, zero]), lanes_of([zero, c1.astype(F32).T]), lanes_of([zero, d.T])]
        )

    def chain_step(level):
        replies["response", level].wait_recv()
        theirs = resp_recv[level]
        if level == last:
            u = fold_rows(dot(tall(theirs), top[0, 1 - top_pos]))
            c1 = top[1, top_pos]
            pack(level, None, None, fold_cols(dot(c1, wide(u))), top[0, top_pos], c1)
            return
        replies["factor", level].wait_recv()
        up = fac_recv[level, :, :rank].astype(BF16)
        sides = fac_recv[level, :, rank:].astype(BF16)
        mixed = fold_rows(dot(tall(theirs), sides))
        lifted = fold_cols(dot(up, wide(mixed)))
        own = fold_rows(dot(tall(resp_send[level]), factor(0, level, 1)))
        own = fold_cols(dot(factor(1, level, 0).astype(F32).T.astype(BF16), wide(own)))
        send_response(level + 1, own + lifted[:, :rank])
        c1 = factor(1, level, 2)
        crossed = fold_cols(dot(c1, wide(mixed)))
        pack(
            level, lifted[:, rank:], crossed[:, :rank], crossed[:, rank:], factor(0, level, 2), c1
        )

    def setup_cross(first, stop):
        product = None
        for level in range(first, stop):
            value = side_mat[level]
            cross[level] = wide(value if product is None else mm(value, product))
            if level + 1 < stop or first == 1:
                step = down_mat[level]
                product = step if product is None else mm(step, product)
        return product

    def ancestors(i, j):
        while i // 2 != j // 2:
            i, j = leaves + i // 2, leaves + j // 2
        return i, j

    def partial(s, which, i, stop):
        value = local[s, i, which].astype(F32)
        n = leaves + i // 2
        while n != stop:
            value = fold_rows(dot(tall(value), local[s, n, which]))
            n = leaves + n // 2
        return value

    def setup_tree(s):
        size = leaves * rank
        tree[s] = jnp.zeros((2 * size, size), BF16)
        for i in range(leaves):
            for j in range(leaves):
                if i == j:
                    continue
                ni, nj = ancestors(i, j)
                if ni == i:
                    tree[s, block(i), block(j)] = local[s, i, 2]
                    continue
                down = fold_rows(dot(tall(partial(s, 1, i, ni)), local[s, ni, 2]))
                value = combine(dot_nt(tall(down), tall(partial(s, 0, j, nj))))
                hi, lo = split(value)
                tree[s, block(i), block(j)] = hi
                tree[s, pl.ds(size + i * rank, rank), block(j)] = lo

    def setup_near():
        loads["near", 0].wait()
        loads["rhs"].wait()
        for i in range(leaves):
            hi, lo = split(dot(vt[1, i], near[0, i]))
            near_coef[i] = rows_of([vt[0, i], hi, lo])
            rhs_coef[block(i)] = fold_cols(dot(vt[1, i], wide(b_ref[i])))

    def setup_plane():
        size = leaves * rank
        inside = tree[0, :size].astype(F32) + tree[0, size:].astype(F32)
        mixed = rows_of([mm(product_vu(i), inside[i * rank : (i + 1) * rank]) for i in range(leaves)])
        up0, up1 = chains[0, 0].T, chains[1, 0].T
        base_a = rows_of([up0, -mm(up1, mixed)])
        p0 = up_mat[0].T
        up = p0
        for level in range(1, bits):
            up = mm(up_mat[level].T, up)
        out_a[...] = tall(mm(up, base_a))
        out_b[...] = tall(mm(up[rank:, rank:], up1))
        in_a[...] = tall(rows_of([base_a, mm(p0, base_a)]))
        in_b[...] = tall(rows_of([up1, mm(p0[rank:, rank:], up1)]))
        down = setup_cross(1, bits)
        enter[...] = wide(rows_of([down_mat[0], side_mat[0]]))
        down = mm(down, down_mat[0])
        leaf_a[...] = tall(chains[0, 1])
        leaf_b[...] = tall(chains[1, 1])
        fall_a[...] = tall(combine(dot_nt(tall(chains[0, 1]), tall(down[:rank, :rank]))))
        fall_b[...] = tall(combine(dot_nt(tall(chains[1, 1]), tall(down[:, rank:]))))


    def merged(k):
        par = k % 2
        started = []

        def start(src, dst, mask):
            return remote(
                src, dst, jsend_sem.at[par], jrecv_sem.at[par], len(started), mask, started
            )

        def across(level, sibling, own):
            value = lanes_of([sibling, own[:, :rank]])
            return combine(dot(tall(value), cross[level]))

        for i in range(leaves):
            out = dot(near_coef[i], xw[i])
            a = fold_cols(out[:rank])
            near_part = out[rank : 2 * rank, :columns] + (
                out[rank : 2 * rank, columns:] + out[2 * rank :, :columns]
            )
            stack[0, block(i)] = wide(a)
            stack[1, block(i)] = wide(rhs_coef[block(i)] - near_part)
        outer = combine(dot(out_a[...], stack[0]))
        outer_b = outer[rank:] + combine(dot(out_b[...], stack[1]))
        outer_t = lanes_of([outer[:rank].T, outer_b.T])
        for j in range(group):
            jw_send[par, j] = outer_t[j * cut : (j + 1) * cut]
        copies_w = []
        for e in range(group - 1, 0, -1):
            copies_w.append(start(jw_send.at[par, member(device(e))], jw_recv.at[par, e], e))

        def inner():
            wide_in = combine(dot(in_a[...], stack[0]))
            narrow = combine(dot(in_b[...], stack[1]))
            jsib[par, 0] = lanes_of([wide_in[:rank].T, (wide_in[rank : 2 * rank] + narrow[:rank]).T])
            jfull[par] = lanes_of(
                [wide_in[2 * rank : 3 * rank].T, (wide_in[3 * rank :] + narrow[rank:]).T]
            )
            copy_a = start(jfull.at[par, pl.ds(other, half)], jr_a.at[par, 0], 1)
            copies_b = [start(jsib.at[par, 0], jsib.at[par, 1], 1)]
            yield
            for level in range(1, bits):
                copy_a.wait_recv()
                if level == 1:
                    value = jfull[par, pl.ds(mine, half)] + jr_a[par, 0]
                else:
                    value = js_a[par, level - 1] + jr_a[par, level - 1]
                if level < bits - 1:
                    js_a[par, level] = combine(dot(tall(value), lift[level]))
                    copy_a = start(js_a.at[par, level], jr_a.at[par, level], 2**level)
                js_b[par, level] = value
                copies_b.append(start(js_b.at[par, level], jr_b.at[par, level], 2**level))
                yield
            far = None
            for level in range(1, bits):
                copies_b[level].wait_recv()
                term = across(level, jr_b[par, level], js_b[par, level])
                far = term if far is None else far + term
            jsib[par, 2, pl.ds(mine, half)] = far
            piece = jsib.at[par, 2, pl.ds(mine, half)]
            copy = start(piece, piece, 1)
            yield
            copies_b[0].wait_recv()
            copy.wait_recv()
            value = lanes_of([jsib[par, 2], jsib[par, 1], jsib[par, 0, :, :rank]])
            value = combine(dot(tall(value), enter[...]))
            field_a[...] = combine(dot_nt(leaf_a[...], tall(value[:, :rank])))
            field_b[...] = combine(dot_nt(leaf_b[...], tall(value[:, rank:])))
            yield

        steps = inner()
        next(steps)
        inside = combine(dot(tree[0], stack[0]))

        def residual(i):
            part = fold_cols(dot(bases[0, i, 0], wide(inside[i * rank : (i + 1) * rank])))
            r_ref[i] = b_ref[i] - fold_cols(dot(near[0, i], xw[i])) - part

        residual(0)
        next(steps)
        for i in range(1, leaves):
            residual(i)
        for copy in copies_w:
            copy.wait_recv()
        value = jw_send[par, me]
        for e in range(1, group):
            value = value + jw_recv[par, e]
        far = None
        for level in range(bits, last - 1):
            jhigh[par, level] = combine(dot(tall(value), lift[level]))
            jhigh[par, levels + level] = value
            copy_a = start(jhigh.at[par, level], jgot.at[par, level], 2**level)
            copy_b = start(
                jhigh.at[par, levels + level], jgot.at[par, levels + 2 + level], 2**level
            )
            copy_a.wait_recv()
            copy_b.wait_recv()
            term = across(level, jgot[par, levels + 2 + level], value)
            far = term if far is None else far + term
            value = jhigh[par, level] + jgot[par, level]
        low, high = last - 1, last
        jhigh[par, high] = combine(dot(tall(value), lift[low]))
        jhigh[par, low] = value
        copies_top = [
            start(jhigh.at[par, src], jgot.at[par, dst], mask)
            for src, dst, mask in (
                (high, high + 1, 2**high + 2**low),
                (high, high, 2**high),
                (high, high + 2, 2**low),
                (low, low, 2**low),
            )
        ]
        for _ in range(bits - 2):
            next(steps)
        copies_top[3].wait_recv()
        term = across(low, jgot[par, low], value)
        far = term if far is None else far + term
        for copy in copies_top[:3]:
            copy.wait_recv()
        own = jhigh[par, high] + jgot[par, high + 2]
        far = far + across(high, jgot[par, high] + jgot[par, high + 1], own)
        jplane[par, pl.ds(my_rows, cut)] = far
        copies_f = []
        for e in range(group - 1, 0, -1):
            piece = jplane.at[par, pl.ds(my_rows, cut)]
            copies_f.append(start(piece, piece, e))
        for _ in steps:
            pass
        for copy in copies_f:
            copy.wait_recv()
        flat = tall(jplane[par])
        alpha = field_a[...] + combine(dot_nt(fall_a[...], flat[:, :rank]))
        sums = None
        for i in range(leaves):
            out = r_ref[i] - fold_cols(dot(bases[0, i, 0], wide(alpha[i * rank : (i + 1) * rank])))
            low_out = out.astype(BF16)
            rb[i] = low_out
            stack[0, block(i)] = wide(dot(vt[1, i], low_out))
            square = jnp.sum((out * out).reshape(-1, 8, columns), axis=0)
            sums = square if sums is None else sums + square
        nrm[pl.ds(k, 1)] = jnp.sum(sums, axis=0, keepdims=True)
        if k == STEPS - 1:
            start_norms()
        beta = field_b[...] + combine(dot_nt(fall_b[...], flat))
        beta = beta + combine(dot(tree[1], stack[0]))
        for i in range(leaves):
            far = beta[i * rank : (i + 1) * rank].astype(BF16)
            value = x_ref[i] + (dot(near[1, i], rb[i]) + dot(bases[1, i, 0], far))
            x_ref[i] = value
            if k < STEPS - 1:
                xw[i] = wide(value)
        for copy in started:
            copy.wait_send()

    norm_copies = []

    def norm_round(index, value):
        lo, hi = norm_rounds(levels)[index]
        nsend[index, pl.ds(0, STEPS)] = value
        copies = []
        for m in range(2 ** (hi - lo) - 1, 0, -1):
            copies.append(
                remote(
                    nsend.at[index, pl.ds(0, STEPS)],
                    nrecv.at[index, m, pl.ds(0, STEPS)],
                    nsend_sem.at[index], nrecv_sem.at[index], m, m << lo, norm_copies,
                )
            )
        return copies

    first_norms = []

    def start_norms():
        first_norms.extend(norm_round(0, nrm[pl.ds(0, STEPS)]))

    def finish_norms():
        copies = first_norms
        for index in range(len(norm_rounds(levels))):
            if index:
                copies = norm_round(index, value)
            for copy in copies:
                copy.wait_recv()
            value = nsend[index, pl.ds(0, STEPS)]
            for m in range(1, len(copies) + 1):
                value = value + nrecv[index, m, pl.ds(0, STEPS)]
        norm_ref[...] = value
        for copy in norm_copies:
            copy.wait_send()

    setup_chain(1)
    setup_up(1)
    loads["res"].wait()
    pl.semaphore_wait(barrier, len(partners))

    def first():
        setup_pairs(1)
        loads["near", 1].wait()
        setup_response()

    def second():
        setup_couplings(1)
        setup_down(1)
        chain_step(0)

    def third():
        loads["top", 0].wait()
        chain_step(1)
        setup_tree(0)

    def fourth():
        setup_tree(1)
        setup_near()

    def fifth():
        for level in range(2, bits):
            chain_step(level)
        setup_plane()

    apply_first([first, second, third, fourth, fifth])
    for level in range(max(2, bits), levels):
        chain_step(level)
    setup_cross(bits, levels)
    for copy in pending:
        copy.wait_send()
    for k in range(STEPS):
        merged(k)
    finish_norms()


def body(right_sides, near_blocks, leaf_bases, local_factors, upper_factors, top_couplings):
    bits_leaf = lax.axis_size("leaf").bit_length() - 1
    bits_rows = lax.axis_size("rows").bit_length() - 1
    levels = bits_leaf + bits_rows
    leaves, size = near_blocks.shape[1], near_blocks.shape[2]
    rank = leaf_bases.shape[4]
    columns = right_sides.shape[1]
    half = columns // 2
    bits = group_bits(levels)
    group = 2**bits
    cut = columns // group
    copies = 2 * (group - 1) + 2 * levels + 4
    nodes = local_factors.shape[1]
    heights = upper_factors.shape[2]
    flat = leaves * rank
    pair = 2 * rank
    rounds = len(norm_rounds(levels))
    vmem = pltpu.VMEM
    dma = pltpu.SemaphoreType.DMA
    out, norms = pl.pallas_call(
        functools.partial(kernel, bits_leaf, bits_rows),
        out_shape=(
            jax.ShapeDtypeStruct((leaves, size, columns), F32),
            jax.ShapeDtypeStruct((STEPS, columns), F32),
        ),
        in_specs=[pl.BlockSpec(memory_space=pl.ANY)] * 6,
        out_specs=(pl.BlockSpec(memory_space=vmem), pl.BlockSpec(memory_space=vmem)),
        scratch_shapes=[
            vmem((leaves, size, columns), F32),
            vmem((leaves, size, columns), F32),
            vmem((2, leaves, size, size), BF16),
            vmem((2, leaves, 2, size, rank), BF16),
            vmem((2, nodes, 3, rank, rank), BF16),
            vmem((2, heights, 3, rank, rank), BF16),
            vmem((2, 2, rank, rank), BF16),
            vmem((2, leaves, rank, size), BF16),
            vmem((leaves - 1, rank, 2 * rank), BF16),
            vmem((levels, rank, 2 * rank), BF16),
            vmem((2 * rank, leaves * rank), BF16),
            vmem((2 * leaves * rank, rank), BF16),
            vmem((nodes - 1, rank, 2 * columns), BF16),
            vmem((nodes - 1, rank, columns), F32),
            vmem((8, columns), F32),
            vmem((group, cut, rank), F32),
            vmem((group, cut, rank), F32),
            vmem((2 * levels, cut, rank), F32),
            vmem((2 * levels + 1, cut, rank), F32),
            vmem((columns, rank), F32),
            vmem((bits, half, rank), F32),
            vmem((bits, half, rank), F32),
            vmem((bits, half, rank), F32),
            vmem((bits, half, rank), F32),
            vmem((3, rank, columns), F32),
            vmem((columns, rank), F32),
            vmem((levels - 1, rank, 3 * rank), F32),
            vmem((levels - 1, rank, 3 * rank), F32),
            vmem((levels, rank, rank), F32),
            vmem((levels, rank, rank), F32),
            vmem((levels, pair, pair), F32),
            vmem((levels, pair, pair), F32),
            vmem((levels, 3 * rank, pair), F32),
            vmem((2, 2, flat, rank), F32),
            vmem((leaves, 3 * rank, size), BF16),
            vmem((flat, columns), F32),
            vmem((2, 2 * flat, flat), BF16),
            vmem((2, flat, 2 * columns), BF16),
            vmem((2 * pair, flat), BF16),
            vmem((pair, flat), BF16),
            vmem((4 * pair, flat), BF16),
            vmem((2 * pair, flat), BF16),
            vmem((levels, pair, 2 * pair), BF16),
            vmem((levels, 3 * rank, 2 * pair), BF16),
            vmem((5 * rank, 2 * pair), BF16),
            vmem((2 * flat, rank), BF16),
            vmem((2 * flat, pair), BF16),
            vmem((2 * flat, rank), BF16),
            vmem((2 * flat, rank), BF16),
            vmem((leaves, size, 2 * columns), BF16),
            vmem((leaves, size, columns), BF16),
            vmem((flat, columns), F32),
            vmem((flat, columns), F32),
            vmem((2, group, cut, pair), F32),
            vmem((2, group, cut, pair), F32),
            vmem((2, 2 * levels, cut, pair), F32),
            vmem((2, 2 * levels + 2, cut, pair), F32),
            vmem((2, columns, pair), F32),
            vmem((2, bits, half, pair), F32),
            vmem((2, bits, half, pair), F32),
            vmem((2, bits, half, pair), F32),
            vmem((2, bits, half, pair), F32),
            vmem((2, 3, columns, pair), F32),
            vmem((2, columns, pair), F32),
            vmem((rounds, 8, columns), F32),
            vmem((rounds, 32, 8, columns), F32),
            dma((12,)),
            dma((copies,)),
            dma((copies,)),
            dma((2, copies)),
            dma((2, copies)),
            dma((2 * levels,)),
            dma((2 * levels,)),
            dma((rounds, 32)),
            dma((rounds, 32)),
        ],
        compiler_params=pltpu.CompilerParams(
            collective_id=0, has_side_effects=True, vmem_limit_bytes=67043328
        ),
    )(
        right_sides.reshape(leaves, size, columns),
        near_blocks,
        leaf_bases,
        local_factors,
        upper_factors,
        top_couplings,
    )
    return out.reshape(-1, columns), norms


def solution(mesh):
    placed = (
        P(("rows", "leaf"), None),
        P(None, ("rows", "leaf"), None, None),
        P(None, ("rows", "leaf"), None, None, None),
        P(None, ("rows", "leaf"), None, None, None),
        P(None, ("rows", "leaf"), None, None, None, None),
        P(),
    )
    return jax.shard_map(
        body,
        mesh=mesh,
        in_specs=placed,
        out_specs=(P(("rows", "leaf"), None), P()),
        check_vma=False,
    )
```

```python
import functools
import jax
import jax.numpy as jnp
from jax import lax
from jax.experimental import pallas as pl
from jax.experimental.pallas import tpu as pltpu
from jax.sharding import PartitionSpec as P

STEPS = 3
F32 = jnp.float32
BF16 = jnp.bfloat16
NT = (((1,), (1,)), ((), ()))


def dot(a, b):
    return jnp.dot(a, b, preferred_element_type=F32)


def split(v):
    hi = v.astype(BF16)
    lo = (v - hi.astype(F32)).astype(BF16)
    return hi, lo


def wide(v):
    return jnp.concatenate(split(v), axis=1)


def tall(v):
    return jnp.concatenate(split(v), axis=0)


def fold_cols(v):
    n = v.shape[1] // 2
    return v[:, :n] + v[:, n:]


def fold_rows(v):
    n = v.shape[0] // 2
    return v[:n] + v[n:]


def combine(out):
    n, m = out.shape[0] // 2, out.shape[1] // 2
    return out[:n, :m] + (out[:n, m:] + out[n:, :m])


def mm(a, b):
    return combine(dot(tall(a), wide(b)))


def dot_nt(a, b):
    return lax.dot_general(a, b, NT, preferred_element_type=F32)


def rows_of(parts):
    return jnp.concatenate(parts, axis=0)


def lanes_of(parts):
    return jnp.concatenate(parts, axis=1)


def norm_rounds(levels):
    return [(lo, min(lo + 5, levels)) for lo in range(0, levels, 5)]


def group_bits(levels):
    return min(3, levels - 2)


def kernel(
    bits_leaf, bits_rows,
    rhs_hbm, near_hbm, bases_hbm, local_hbm, upper_hbm, top_hbm,
    x_ref, norm_ref,
    b_ref, r_ref, near, bases, local, upper, top,
    vt, pt, tt, et, jt, cb, pre, nrm,
    w_send, w_recv, high_a, got_a, plane,
    send_a, send_b, recv_a, recv_b, sib_full, full,
    fac_send, fac_recv, resp_send, resp_recv,
    up_mat, down_mat, side_mat,
    gram, base_a, base_b,
    chains, near_coef, rhs_coef, tree, stack,
    out_a, out_b, in_a, in_b, lift, cross, enter,
    fall_a, fall_b, leaf_a, leaf_b, xw, rb, field_a, field_b,
    jw_send, jw_recv, jhigh, jgot, jplane,
    js_a, js_b, jr_a, jr_b, jsib, jfull,
    nsend, nrecv,
    load_sem, send_sem, recv_sem, fsend_sem, frecv_sem, nsend_sem, nrecv_sem,
):
    leaves = near.shape[1]
    levels = bits_leaf + bits_rows
    last = levels - 1
    bits = group_bits(levels)
    group = 2**bits
    root = 2 * leaves - 2
    leaf = lax.axis_index("leaf")
    rows = lax.axis_index("rows")
    columns = x_ref.shape[2]
    rank = plane.shape[1]
    half = columns // 2
    cut = columns // group
    mine = pl.multiple_of(leaf % 2 * half, half)
    other = pl.multiple_of((1 - leaf % 2) * half, half)
    top_pos = rows // 2 ** (bits_rows - 1)

    def flipped(value, mask):
        for bit in range(mask.bit_length()):
            d = 2**bit
            if mask & d:
                value = value + d - 2 * d * (value // d % 2)
        return value

    def device(mask):
        leaf_mask = mask % 2**bits_leaf
        return (flipped(rows, mask // 2**bits_leaf), flipped(leaf, leaf_mask))

    def member(place):
        row, column = place
        if bits <= bits_leaf:
            return column % group
        return column + 2**bits_leaf * (row % 2 ** (bits - bits_leaf))

    me = member((rows, leaf))
    my_rows = pl.multiple_of(me * cut, cut)

    def load(src, dst, index):
        return pltpu.make_async_copy(src, dst, load_sem.at[index])

    loads = {}
    order = []
    for s in (1, 0):
        order += [
            (("local", s), local_hbm.at[s], local.at[s]),
            (("upper", s), upper_hbm.at[s, 0], upper.at[s]),
            (("bases", s), bases_hbm.at[s], bases.at[s]),
        ]
        if s == 1:
            order += [("res", rhs_hbm, r_ref)]
        order += [
            (("near", s), near_hbm.at[s], near.at[s]),
            (("top", s), top_hbm.at[s], top.at[s]),
        ]
        if s == 1:
            order += [("rhs", rhs_hbm, b_ref)]
    for index, (name, src, dst) in enumerate(order):
        loads[name] = load(src, dst, index)
        loads[name].start()

    barrier = pltpu.get_barrier_semaphore()
    partners = set(range(1, group)) | {2**level for level in range(levels)}
    partners.add(2**last + 2 ** (last - 1))
    partners = sorted(partners)
    for mask in partners:
        pl.semaphore_signal(
            barrier, inc=1, device_id=device(mask), device_id_type=pl.DeviceIdType.MESH
        )

    def remote(src, dst, sends, recvs, index, mask, started):
        copy = pltpu.make_async_remote_copy(
            src_ref=src,
            dst_ref=dst,
            send_sem=sends.at[index],
            recv_sem=recvs.at[index],
            device_id=device(mask),
            device_id_type=pl.DeviceIdType.MESH,
        )
        copy.start()
        started.append(copy)
        return copy

    def block(i, n=1):
        return pl.ds(i * rank, n * rank)

    def factor(s, level, which):
        return local[s, root, which] if level == 0 else upper[s, level - 1, which]


    def chain(s, which):
        product = upper[s, bits - 2, which].astype(F32)
        for index in range(bits - 3, -1, -1):
            product = fold_cols(dot(upper[s, index, which], wide(product)))
        node = {root: fold_cols(dot(local[s, root, which], wide(product)))}
        for n in range(root - 1, -1, -1):
            parent = leaves + n // 2
            node[n] = fold_cols(dot(local[s, n, which], wide(node[parent])))
        return [node[i] for i in range(leaves)]

    def setup_chain(s):
        loads["local", s].wait()
        loads["upper", s].wait()
        et[...] = tall(lanes_of([v.T for v in chain(s, 0)]))

    def setup_up(s):
        loads["bases", s].wait()
        for i in range(leaves):
            vt[s, i] = bases[s, i, 1].astype(F32).T.astype(BF16)

    def setup_pairs(s):
        for p in range(leaves - 1):
            pair = [local[s, 2 * p + j, 0].astype(F32).T.astype(BF16) for j in range(2)]
            pt[p] = lanes_of(pair)

    def setup_couplings(s):
        loads["top", s].wait()
        for first, stop in ((1, bits), (bits, levels)):
            product = None
            for level in range(first, stop):
                coupling = top[s, top_pos] if level == last else upper[s, level - 1, 2]
                if product is None:
                    value = coupling.astype(F32)
                else:
                    value = fold_rows(dot(tall(product), coupling))
                tt[level] = wide(value.T)
                if level + 1 < stop:
                    q = upper[s, level - 1, 1]
                    product = q.astype(F32) if product is None else fold_rows(dot(tall(product), q))

    def setup_down(s):
        jt[...] = tall(rows_of(chain(s, 1)))

    def apply_first(prepare, hooks):
        s = 1
        started = []
        hooks = list(hooks)

        def start(src, dst, mask):
            return remote(src, dst, send_sem, recv_sem.at[1], len(started), mask, started)

        def across(value, level):
            return combine(dot(tall(value), tt[level]))

        def near_leaf(i):
            x_ref[i] = dot(near[s, i], r_ref[i].astype(BF16))

        def couple(n):
            sibling = n + 1 - 2 * (n % 2)
            pre[n] = fold_cols(dot(local[s, n, 2], cb[sibling]))

        field = {}

        def inner():
            for p in range(leaves - 1):
                stacked = rows_of([cb[2 * p], cb[2 * p + 1]])
                coefficient = fold_cols(dot(pt[p], stacked))
                if p < leaves - 2:
                    cb[leaves + p] = wide(coefficient)
            full[...] = fold_rows(dot(tall(coefficient.T), local[s, root, 0]))
            sib_full[0] = coefficient
            copy_a = start(full.at[pl.ds(other, half)], recv_a.at[0], 1)
            copies_b = [start(sib_full.at[0], sib_full.at[1], 1)]
            yield
            for level in range(1, bits):
                copy_a.wait_recv()
                if level == 1:
                    value = full[pl.ds(mine, half)] + recv_a[0]
                else:
                    value = send_a[level - 1] + recv_a[level - 1]
                if level < bits - 1:
                    send_a[level] = fold_rows(dot(tall(value), upper[s, level - 1, 0]))
                    copy_a = start(send_a.at[level], recv_a.at[level], 2**level)
                send_b[level] = value
                copies_b.append(start(send_b.at[level], recv_b.at[level], 2**level))
                if level == 1:
                    for n in range(root):
                        couple(n)
                    copies_b[0].wait_recv()
                    root_pre = fold_cols(dot(local[s, root, 2], wide(sib_full[1])))
                yield
            far = None
            for level in range(1, bits):
                copies_b[level].wait_recv()
                term = across(recv_b[level], level)
                far = term if far is None else far + term
            sib_full[2, pl.ds(mine, half)] = far
            piece = sib_full.at[2, pl.ds(mine, half)]
            copy = start(piece, piece, 1)
            yield
            copy.wait_recv()
            product = dot_nt(local[s, root, 1], tall(sib_full[2]))
            field[root] = fold_cols(product) + root_pre
            for n in range(root - 1, -1, -1):
                parent = leaves + n // 2
                field[n] = fold_cols(dot(local[s, n, 1], wide(field[parent]))) + pre[n]
            yield

        for i in range(leaves):
            cb[i] = wide(dot(vt[s, i], r_ref[i].astype(BF16)))
        stacked = rows_of([cb[i] for i in range(leaves)])
        outer_t = combine(dot(et[...], stacked)).T
        for j in range(group):
            w_send[j] = outer_t[j * cut : (j + 1) * cut]
        prepare()
        copies_w = []
        for e in range(group - 1, 0, -1):
            copies_w.append(start(w_send.at[member(device(e))], w_recv.at[e], e))
        steps = inner()
        work = list(range(leaves))

        def fill(everything=False):
            if hooks:
                hooks.pop(0)()
            next(steps, None)
            while work:
                near_leaf(work.pop(0))
                if not everything:
                    break

        fill()
        fill()
        for copy in copies_w:
            copy.wait_recv()
        value = w_send[me]
        for e in range(1, group):
            value = value + w_recv[e]
        far = None
        for level in range(bits, last - 1):
            high_a[level] = fold_rows(dot(tall(value), upper[s, level - 1, 0]))
            high_a[levels + level] = value
            copy_a = start(high_a.at[level], got_a.at[level], 2**level)
            copy_b = start(high_a.at[levels + level], got_a.at[levels + 1 + level], 2**level)
            fill()
            copy_a.wait_recv()
            value = high_a[level] + got_a[level]
            copy_b.wait_recv()
            term = across(got_a[levels + 1 + level], level)
            far = term if far is None else far + term
        low, high = last - 1, last
        high_a[high] = fold_rows(dot(tall(value), upper[s, low - 1, 0]))
        high_a[low] = value
        copies_top = [
            start(high_a.at[src], got_a.at[dst], mask)
            for src, dst, mask in (
                (high, high + 1, 2**high + 2**low),
                (high, high, 2**high),
                (low, low, 2**low),
            )
        ]
        fill()
        copies_top[2].wait_recv()
        term = across(got_a[low], low)
        far = term if far is None else far + term
        fill(True)
        copies_top[1].wait_recv()
        copies_top[0].wait_recv()
        far = far + across(got_a[high] + got_a[high + 1], high)
        plane[pl.ds(my_rows, cut)] = far
        copies_f = []
        for e in range(group - 1, 0, -1):
            piece = plane.at[pl.ds(my_rows, cut)]
            copies_f.append(start(piece, piece, e))
        for _ in steps:
            pass
        while hooks:
            hooks.pop(0)()
        for copy in copies_f:
            copy.wait_recv()
        outer = combine(dot_nt(jt[...], tall(plane[...])))
        for i in range(leaves):
            total = field[i] + outer[i * rank : (i + 1) * rank]
            value = x_ref[i] + dot(bases[s, i, 0], total.astype(BF16))
            x_ref[i] = value
            xw[i] = wide(value)
        for copy in started:
            copy.wait_send()


    pending = []
    own_part = {}
    replies = {}

    def local_chain(s, which):
        node = {}
        for n in range(root - 1, -1, -1):
            parent = leaves + n // 2
            own = local[s, n, which]
            if parent == root:
                node[n] = own.astype(F32)
            else:
                node[n] = fold_cols(dot(own, wide(node[parent])))
        return rows_of([node[i] for i in range(leaves)])

    def send_response(level, value):
        if value is not None:
            resp_send[level] = value
        replies["response", level] = remote(
            resp_send.at[level], resp_recv.at[level], fsend_sem, frecv_sem,
            levels + level, 2**level, pending,
        )

    def lift_response(level):
        own = fold_rows(dot(tall(resp_send[level]), factor(0, level, 1)))
        up = fac_send[level, :, :rank].astype(BF16)
        own_part[level] = fold_cols(dot(up, wide(own)))

    def prepare_response():
        loads["local", 0].wait()
        loads["upper", 0].wait()
        setup_up(0)
        for s in range(2):
            for which in range(2):
                chains[s, which] = local_chain(s, which)
        for i in range(leaves):
            gram[block(i)] = dot(vt[1, i], bases[0, i, 0])
        middle = rows_of([mm(gram[block(i)], chains[0, 1, block(i)]) for i in range(leaves)])
        resp_send[0] = -mm(chains[1, 0].T, middle)
        for level in range(last):
            fac_send[level] = lanes_of(
                [
                    factor(1, level, 0).astype(F32).T,
                    factor(0, level, 1).astype(F32),
                    factor(0, level, 2).astype(F32),
                ]
            )

    def send_factors(which):
        for level in which:
            replies["factor", level] = remote(
                fac_send.at[level], fac_recv.at[level], fsend_sem, frecv_sem,
                level, 2**level, pending,
            )

    def pack(level, x, y, d, c0, c1):
        zero = jnp.zeros((rank, rank), F32)
        if x is not None:
            p = [factor(s, level, 0).astype(F32) for s in range(2)]
            q = [factor(s, level, 1).astype(F32).T for s in range(2)]
            up_mat[level] = rows_of([lanes_of([p[0], x.T]), lanes_of([zero, p[1]])])
            down_mat[level] = rows_of([lanes_of([q[0], y.T]), lanes_of([zero, q[1]])])
            lift[level] = wide(up_mat[level])
        side_mat[level] = rows_of(
            [lanes_of([c0.astype(F32).T, zero]), lanes_of([zero, c1.astype(F32).T]), lanes_of([zero, d.T])]
        )

    def chain_step(level):
        replies["response", level].wait_recv()
        theirs = resp_recv[level]
        if level == last:
            u = fold_rows(dot(tall(theirs), top[0, 1 - top_pos]))
            c1 = top[1, top_pos]
            pack(level, None, None, fold_cols(dot(c1, wide(u))), top[0, top_pos], c1)
            return
        replies["factor", level].wait_recv()
        up = fac_recv[level, :, :rank].astype(BF16)
        sides = fac_recv[level, :, rank:].astype(BF16)
        mixed = fold_rows(dot(tall(theirs), sides))
        lifted = fold_cols(dot(up, wide(mixed)))
        send_response(level + 1, own_part[level] + lifted[:, :rank])
        if level + 1 < last:
            lift_response(level + 1)
        c1 = factor(1, level, 2)
        crossed = fold_cols(dot(c1, wide(mixed)))
        pack(
            level, lifted[:, rank:], crossed[:, :rank], crossed[:, rank:], factor(0, level, 2), c1
        )

    def setup_cross(first, stop):
        product = None
        for level in range(first, stop):
            value = side_mat[level]
            cross[level] = wide(value if product is None else mm(value, product))
            if level + 1 < stop or first == 1:
                step = down_mat[level]
                product = step if product is None else mm(step, product)
        return product

    def ancestors(i, j):
        while i // 2 != j // 2:
            i, j = leaves + i // 2, leaves + j // 2
        return i, j

    def partial(s, which, i, stop):
        value = local[s, i, which].astype(F32)
        n = leaves + i // 2
        while n != stop:
            value = fold_rows(dot(tall(value), local[s, n, which]))
            n = leaves + n // 2
        return value

    def setup_tree(s):
        size = leaves * rank
        tree[s] = jnp.zeros((2 * size, size), BF16)
        for i in range(leaves):
            for j in range(leaves):
                if i == j:
                    continue
                ni, nj = ancestors(i, j)
                if ni == i:
                    tree[s, block(i), block(j)] = local[s, i, 2]
                    continue
                down = fold_rows(dot(tall(partial(s, 1, i, ni)), local[s, ni, 2]))
                value = combine(dot_nt(tall(down), tall(partial(s, 0, j, nj))))
                hi, lo = split(value)
                tree[s, block(i), block(j)] = hi
                tree[s, pl.ds(size + i * rank, rank), block(j)] = lo

    def setup_near():
        loads["near", 0].wait()
        loads["rhs"].wait()
        for i in range(leaves):
            hi, lo = split(dot(vt[1, i], near[0, i]))
            near_coef[i] = rows_of([vt[0, i], hi, lo])
            rhs_coef[block(i)] = fold_cols(dot(vt[1, i], wide(b_ref[i])))

    def setup_base():
        size = leaves * rank
        inside = tree[0, :size].astype(F32) + tree[0, size:].astype(F32)
        mixed = rows_of([mm(gram[block(i)], inside[i * rank : (i + 1) * rank]) for i in range(leaves)])
        up0, up1 = chains[0, 0].T, chains[1, 0].T
        base_a[...] = rows_of([up0, -mm(up1, mixed)])
        base_b[...] = up1

    def setup_rise():
        up = up_mat[0].T
        for level in range(1, bits):
            up = mm(up_mat[level].T, up)
        out_a[...] = tall(mm(up, base_a[...]))
        out_b[...] = tall(mm(up[rank:, rank:], base_b[...]))

    def setup_enter():
        p0 = up_mat[0].T
        in_a[...] = tall(rows_of([base_a[...], mm(p0, base_a[...])]))
        in_b[...] = tall(rows_of([base_b[...], mm(p0[rank:, rank:], base_b[...])]))

    def setup_fall():
        down = setup_cross(1, bits)
        enter[...] = wide(rows_of([down_mat[0], side_mat[0]]))
        down = mm(down, down_mat[0])
        leaf_a[...] = tall(chains[0, 1])
        leaf_b[...] = tall(chains[1, 1])
        fall_a[...] = tall(combine(dot_nt(tall(chains[0, 1]), tall(down[:rank, :rank]))))
        fall_b[...] = tall(combine(dot_nt(tall(chains[1, 1]), tall(down[:, rank:]))))


    def merged(k, hooks):
        par = k % 2
        started = []
        hooks = list(hooks)

        def hook():
            if hooks:
                hooks.pop(0)()

        def start(src, dst, mask):
            return remote(
                src, dst, send_sem, recv_sem.at[par], len(started), mask, started
            )

        def across(level, sibling, own):
            value = lanes_of([sibling, own[:, :rank]])
            return combine(dot(tall(value), cross[level]))

        for i in range(leaves):
            out = dot(near_coef[i], xw[i])
            a = fold_cols(out[:rank])
            near_part = out[rank : 2 * rank, :columns] + (
                out[rank : 2 * rank, columns:] + out[2 * rank :, :columns]
            )
            stack[0, block(i)] = wide(a)
            stack[1, block(i)] = wide(rhs_coef[block(i)] - near_part)
        outer = combine(dot(out_a[...], stack[0]))
        outer_b = outer[rank:] + combine(dot(out_b[...], stack[1]))
        outer_t = lanes_of([outer[:rank].T, outer_b.T])
        for j in range(group):
            jw_send[par, j] = outer_t[j * cut : (j + 1) * cut]
        copies_w = []
        for e in range(group - 1, 0, -1):
            copies_w.append(start(jw_send.at[par, member(device(e))], jw_recv.at[par, e], e))

        hook()

        def inner():
            wide_in = combine(dot(in_a[...], stack[0]))
            narrow = combine(dot(in_b[...], stack[1]))
            jsib[par, 0] = lanes_of([wide_in[:rank].T, (wide_in[rank : 2 * rank] + narrow[:rank]).T])
            jfull[par] = lanes_of(
                [wide_in[2 * rank : 3 * rank].T, (wide_in[3 * rank :] + narrow[rank:]).T]
            )
            copy_a = start(jfull.at[par, pl.ds(other, half)], jr_a.at[par, 0], 1)
            copies_b = [start(jsib.at[par, 0], jsib.at[par, 1], 1)]
            yield
            for level in range(1, bits):
                copy_a.wait_recv()
                if level == 1:
                    value = jfull[par, pl.ds(mine, half)] + jr_a[par, 0]
                else:
                    value = js_a[par, level - 1] + jr_a[par, level - 1]
                if level < bits - 1:
                    js_a[par, level] = combine(dot(tall(value), lift[level]))
                    copy_a = start(js_a.at[par, level], jr_a.at[par, level], 2**level)
                js_b[par, level] = value
                copies_b.append(start(js_b.at[par, level], jr_b.at[par, level], 2**level))
                yield
            far = None
            for level in range(1, bits):
                copies_b[level].wait_recv()
                term = across(level, jr_b[par, level], js_b[par, level])
                far = term if far is None else far + term
            jsib[par, 2, pl.ds(mine, half)] = far
            piece = jsib.at[par, 2, pl.ds(mine, half)]
            copy = start(piece, piece, 1)
            yield
            copies_b[0].wait_recv()
            copy.wait_recv()
            value = lanes_of([jsib[par, 2], jsib[par, 1], jsib[par, 0, :, :rank]])
            value = combine(dot(tall(value), enter[...]))
            field_a[...] = combine(dot_nt(leaf_a[...], tall(value[:, :rank])))
            field_b[...] = combine(dot_nt(leaf_b[...], tall(value[:, rank:])))
            yield

        steps = inner()
        next(steps)
        inside = combine(dot(tree[0], stack[0]))

        def residual(i):
            part = fold_cols(dot(bases[0, i, 0], wide(inside[i * rank : (i + 1) * rank])))
            r_ref[i] = b_ref[i] - fold_cols(dot(near[0, i], xw[i])) - part

        residual(0)
        next(steps)
        hook()
        for i in range(1, leaves):
            residual(i)
        for copy in copies_w:
            copy.wait_recv()
        value = jw_send[par, me]
        for e in range(1, group):
            value = value + jw_recv[par, e]
        far = None
        for level in range(bits, last - 1):
            jhigh[par, level] = combine(dot(tall(value), lift[level]))
            jhigh[par, levels + level] = value
            copy_a = start(jhigh.at[par, level], jgot.at[par, level], 2**level)
            copy_b = start(
                jhigh.at[par, levels + level], jgot.at[par, levels + 2 + level], 2**level
            )
            copy_a.wait_recv()
            copy_b.wait_recv()
            term = across(level, jgot[par, levels + 2 + level], value)
            far = term if far is None else far + term
            value = jhigh[par, level] + jgot[par, level]
        low, high = last - 1, last
        jhigh[par, high] = combine(dot(tall(value), lift[low]))
        jhigh[par, low] = value
        copies_top = [
            start(jhigh.at[par, src], jgot.at[par, dst], mask)
            for src, dst, mask in (
                (high, high + 1, 2**high + 2**low),
                (high, high, 2**high),
                (high, high + 2, 2**low),
                (low, low, 2**low),
            )
        ]
        for _ in range(bits - 2):
            next(steps)
        hook()
        copies_top[3].wait_recv()
        term = across(low, jgot[par, low], value)
        far = term if far is None else far + term
        for copy in copies_top[:3]:
            copy.wait_recv()
        own = jhigh[par, high] + jgot[par, high + 2]
        far = far + across(high, jgot[par, high] + jgot[par, high + 1], own)
        jplane[par, pl.ds(my_rows, cut)] = far
        copies_f = []
        for e in range(group - 1, 0, -1):
            piece = jplane.at[par, pl.ds(my_rows, cut)]
            copies_f.append(start(piece, piece, e))
        for _ in steps:
            pass
        for copy in copies_f:
            copy.wait_recv()
        flat = tall(jplane[par])
        alpha = field_a[...] + combine(dot_nt(fall_a[...], flat[:, :rank]))
        sums = None
        for i in range(leaves):
            out = r_ref[i] - fold_cols(dot(bases[0, i, 0], wide(alpha[i * rank : (i + 1) * rank])))
            low_out = out.astype(BF16)
            rb[i] = low_out
            stack[0, block(i)] = wide(dot(vt[1, i], low_out))
            square = jnp.sum((out * out).reshape(-1, 8, columns), axis=0)
            sums = square if sums is None else sums + square
        nrm[pl.ds(k, 1)] = jnp.sum(sums, axis=0, keepdims=True)
        if k == STEPS - 1:
            start_norms()
        beta = field_b[...] + combine(dot_nt(fall_b[...], flat))
        beta = beta + combine(dot(tree[1], stack[0]))
        for i in range(leaves):
            far = beta[i * rank : (i + 1) * rank].astype(BF16)
            value = x_ref[i] + (dot(near[1, i], rb[i]) + dot(bases[1, i, 0], far))
            x_ref[i] = value
            if k < STEPS - 1:
                xw[i] = wide(value)
        for copy in started:
            copy.wait_send()

    def norm_round(index, value):
        lo, hi = norm_rounds(levels)[index]
        nsend[index, pl.ds(0, STEPS)] = value
        for m in range(2 ** (hi - lo) - 1, 0, -1):
            pltpu.make_async_remote_copy(
                src_ref=nsend.at[index, pl.ds(0, STEPS)],
                dst_ref=nrecv.at[index, m, pl.ds(0, STEPS)],
                send_sem=nsend_sem.at[index],
                recv_sem=nrecv_sem.at[index],
                device_id=device(m << lo),
                device_id_type=pl.DeviceIdType.MESH,
            ).start()

    def start_norms():
        norm_round(0, nrm[pl.ds(0, STEPS)])

    def finish_norms():
        waits = []
        for index, (lo, hi) in enumerate(norm_rounds(levels)):
            if index:
                norm_round(index, value)
            count = 2 ** (hi - lo)
            every = nrecv.at[index, pl.ds(1, count - 1), pl.ds(0, STEPS)]
            pltpu.make_async_copy(every, every, nrecv_sem.at[index]).wait()
            waits.append(pltpu.make_async_copy(every, every, nsend_sem.at[index]))
            value = nsend[index, pl.ds(0, STEPS)]
            for m in range(1, count):
                value = value + nrecv[index, m, pl.ds(0, STEPS)]
        norm_ref[...] = value
        for copy in waits:
            copy.wait()

    setup_chain(1)
    setup_up(1)
    loads["res"].wait()

    def prepare():
        prepare_response()
        setup_tree(0)
        pl.semaphore_wait(barrier, len(partners))

    def first():
        send_response(0, None)
        send_factors([level for level in range(last) if level != 1])
        lift_response(0)
        setup_pairs(1)
        loads["near", 1].wait()

    def second():
        chain_step(0)
        setup_couplings(1)
        setup_down(1)

    def third():
        send_factors([1])
        loads["top", 0].wait()
        setup_near()

    def fourth():
        chain_step(1)

    def fifth():
        setup_base()
        for level in range(2, bits):
            chain_step(level)
        setup_rise()

    def sixth():
        setup_tree(1)
        for level in range(bits, last):
            chain_step(level)

    def seventh():
        setup_fall()
        chain_step(last)
        setup_cross(bits, levels)
        for copy in pending:
            copy.wait_send()

    apply_first(prepare, [first, second, third, fourth, fifth])
    merged(0, [setup_enter, sixth, seventh])
    for k in range(1, STEPS):
        merged(k, [lambda: None])
    finish_norms()


def body(right_sides, near_blocks, leaf_bases, local_factors, upper_factors, top_couplings):
    bits_leaf = lax.axis_size("leaf").bit_length() - 1
    bits_rows = lax.axis_size("rows").bit_length() - 1
    levels = bits_leaf + bits_rows
    leaves, size = near_blocks.shape[1], near_blocks.shape[2]
    rank = leaf_bases.shape[4]
    columns = right_sides.shape[1]
    half = columns // 2
    bits = group_bits(levels)
    group = 2**bits
    cut = columns // group
    copies = 2 * (group - 1) + 2 * bits + 2 * (levels - 2 - bits) + 4
    nodes = local_factors.shape[1]
    heights = upper_factors.shape[2]
    flat = leaves * rank
    pair = 2 * rank
    rounds = len(norm_rounds(levels))
    vmem = pltpu.VMEM
    dma = pltpu.SemaphoreType.DMA
    out, norms = pl.pallas_call(
        functools.partial(kernel, bits_leaf, bits_rows),
        out_shape=(
            vmem((leaves, size, columns), F32),
            vmem((STEPS, columns), F32),
        ),
        in_specs=[pl.BlockSpec(memory_space=pl.ANY)] * 6,
        out_specs=(pl.BlockSpec(memory_space=vmem), pl.BlockSpec(memory_space=vmem)),
        scratch_shapes=[
            vmem((leaves, size, columns), F32),
            vmem((leaves, size, columns), F32),
            vmem((2, leaves, size, size), BF16),
            vmem((2, leaves, 2, size, rank), BF16),
            vmem((2, nodes, 3, rank, rank), BF16),
            vmem((2, heights, 3, rank, rank), BF16),
            vmem((2, 2, rank, rank), BF16),
            vmem((2, leaves, rank, size), BF16),
            vmem((leaves - 1, rank, 2 * rank), BF16),
            vmem((levels, rank, 2 * rank), BF16),
            vmem((2 * rank, leaves * rank), BF16),
            vmem((2 * leaves * rank, rank), BF16),
            vmem((nodes - 1, rank, 2 * columns), BF16),
            vmem((nodes - 1, rank, columns), F32),
            vmem((8, columns), F32),
            vmem((group, cut, rank), F32),
            vmem((group, cut, rank), F32),
            vmem((2 * levels, cut, rank), F32),
            vmem((2 * levels + 1, cut, rank), F32),
            vmem((columns, rank), F32),
            vmem((bits, half, rank), F32),
            vmem((bits, half, rank), F32),
            vmem((bits, half, rank), F32),
            vmem((bits, half, rank), F32),
            vmem((3, rank, columns), F32),
            vmem((columns, rank), F32),
            vmem((levels - 1, rank, 3 * rank), F32),
            vmem((levels - 1, rank, 3 * rank), F32),
            vmem((levels, rank, rank), F32),
            vmem((levels, rank, rank), F32),
            vmem((levels, pair, pair), F32),
            vmem((levels, pair, pair), F32),
            vmem((levels, 3 * rank, pair), F32),
            vmem((flat, rank), F32),
            vmem((pair, flat), F32),
            vmem((rank, flat), F32),
            vmem((2, 2, flat, rank), F32),
            vmem((leaves, 3 * rank, size), BF16),
            vmem((flat, columns), F32),
            vmem((2, 2 * flat, flat), BF16),
            vmem((2, flat, 2 * columns), BF16),
            vmem((2 * pair, flat), BF16),
            vmem((pair, flat), BF16),
            vmem((4 * pair, flat), BF16),
            vmem((2 * pair, flat), BF16),
            vmem((levels, pair, 2 * pair), BF16),
            vmem((levels, 3 * rank, 2 * pair), BF16),
            vmem((5 * rank, 2 * pair), BF16),
            vmem((2 * flat, rank), BF16),
            vmem((2 * flat, pair), BF16),
            vmem((2 * flat, rank), BF16),
            vmem((2 * flat, rank), BF16),
            vmem((leaves, size, 2 * columns), BF16),
            vmem((leaves, size, columns), BF16),
            vmem((flat, columns), F32),
            vmem((flat, columns), F32),
            vmem((2, group, cut, pair), F32),
            vmem((2, group, cut, pair), F32),
            vmem((2, 2 * levels, cut, pair), F32),
            vmem((2, 2 * levels + 2, cut, pair), F32),
            vmem((2, columns, pair), F32),
            vmem((2, bits, half, pair), F32),
            vmem((2, bits, half, pair), F32),
            vmem((2, bits, half, pair), F32),
            vmem((2, bits, half, pair), F32),
            vmem((2, 3, columns, pair), F32),
            vmem((2, columns, pair), F32),
            vmem((rounds, 8, columns), F32),
            vmem((rounds, 32, 8, columns), F32),
            dma((12,)),
            dma((copies,)),
            dma((2, copies)),
            dma((2 * levels,)),
            dma((2 * levels,)),
            dma((rounds,)),
            dma((rounds,)),
        ],
        compiler_params=pltpu.CompilerParams(
            collective_id=0, has_side_effects=True, vmem_limit_bytes=60000000
        ),
    )(
        right_sides.reshape(leaves, size, columns),
        near_blocks,
        leaf_bases,
        local_factors,
        upper_factors,
        top_couplings,
    )
    return out.reshape(-1, columns), norms


def solution(mesh):
    placed = (
        P(("rows", "leaf"), None),
        P(None, ("rows", "leaf"), None, None),
        P(None, ("rows", "leaf"), None, None, None),
        P(None, ("rows", "leaf"), None, None, None),
        P(None, ("rows", "leaf"), None, None, None, None),
        P(),
    )
    return jax.shard_map(
        body,
        mesh=mesh,
        in_specs=placed,
        out_specs=(P(("rows", "leaf"), None), P()),
        check_vma=False,
    )
```

```python
import functools
import jax
import jax.numpy as jnp
from jax import lax
from jax.experimental import pallas as pl
from jax.experimental.pallas import tpu as pltpu
from jax.sharding import PartitionSpec as P

STEPS = 3
F32 = jnp.float32
BF16 = jnp.bfloat16
NT = (((1,), (1,)), ((), ()))


def dot(a, b):
    return jnp.dot(a, b, preferred_element_type=F32)


def split(v):
    hi = v.astype(BF16)
    lo = (v - hi.astype(F32)).astype(BF16)
    return hi, lo


def wide(v):
    return jnp.concatenate(split(v), axis=1)


def tall(v):
    return jnp.concatenate(split(v), axis=0)


def fold_cols(v):
    n = v.shape[1] // 2
    return v[:, :n] + v[:, n:]


def fold_rows(v):
    n = v.shape[0] // 2
    return v[:n] + v[n:]


def combine(out):
    n, m = out.shape[0] // 2, out.shape[1] // 2
    return out[:n, :m] + (out[:n, m:] + out[n:, :m])


def mm(a, b):
    return combine(dot(tall(a), wide(b)))


def dot_nt(a, b):
    return lax.dot_general(a, b, NT, preferred_element_type=F32)


def rows_of(parts):
    return jnp.concatenate(parts, axis=0)


def lanes_of(parts):
    return jnp.concatenate(parts, axis=1)


def norm_rounds(levels):
    return [(lo, min(lo + 5, levels)) for lo in range(0, levels, 5)]


def group_bits(levels):
    return min(3, levels - 2)


def kernel(
    bits_leaf, bits_rows,
    rhs_hbm, near_hbm, bases_hbm, local_hbm, upper_hbm, top_hbm,
    x_ref, norm_ref,
    b_ref, r_ref, near, bases, local, upper, top,
    vt, pt, tt, et, jt, cb, pre, nrm,
    w_send, w_recv, high_a, got_a, plane,
    send_a, send_b, recv_a, recv_b, sib_full, full,
    fac_send, fac_recv, resp_send, resp_recv,
    up_mat, down_mat, side_mat,
    gram, base_a, base_b,
    chains, near_coef, rhs_coef, tree, stack,
    out_a, out_b, in_a, in_b, lift, cross, enter,
    fall_a, fall_b, leaf_a, leaf_b, xw, rb, field_a, field_b,
    jw_send, jw_recv, jhigh, jgot, jplane,
    js_a, js_b, jr_a, jr_b, jsib, jfull,
    nsend, nrecv,
    load_sem, send_sem, recv_sem, fsend_sem, frecv_sem, nsend_sem, nrecv_sem,
):
    leaves = near.shape[1]
    levels = bits_leaf + bits_rows
    last = levels - 1
    bits = group_bits(levels)
    group = 2**bits
    root = 2 * leaves - 2
    leaf = lax.axis_index("leaf")
    rows = lax.axis_index("rows")
    columns = x_ref.shape[2]
    rank = plane.shape[1]
    half = columns // 2
    cut = columns // group
    mine = pl.multiple_of(leaf % 2 * half, half)
    other = pl.multiple_of((1 - leaf % 2) * half, half)
    top_pos = rows // 2 ** (bits_rows - 1)

    def flipped(value, mask):
        for bit in range(mask.bit_length()):
            d = 2**bit
            if mask & d:
                value = value + d - 2 * d * (value // d % 2)
        return value

    def device(mask):
        leaf_mask = mask % 2**bits_leaf
        return (flipped(rows, mask // 2**bits_leaf), flipped(leaf, leaf_mask))

    def member(place):
        row, column = place
        if bits <= bits_leaf:
            return column % group
        return column + 2**bits_leaf * (row % 2 ** (bits - bits_leaf))

    me = member((rows, leaf))
    my_rows = pl.multiple_of(me * cut, cut)

    def load(src, dst, index):
        return pltpu.make_async_copy(src, dst, load_sem.at[index])

    loads = {}
    order = []
    for s in (1, 0):
        order += [
            (("local", s), local_hbm.at[s], local.at[s]),
            (("upper", s), upper_hbm.at[s, 0], upper.at[s]),
            (("bases", s), bases_hbm.at[s], bases.at[s]),
        ]
        if s == 1:
            order += [("res", rhs_hbm, r_ref)]
        order += [
            (("near", s), near_hbm.at[s], near.at[s]),
            (("top", s), top_hbm.at[s], top.at[s]),
        ]
        if s == 1:
            order += [("rhs", rhs_hbm, b_ref)]
    for index, (name, src, dst) in enumerate(order):
        loads[name] = load(src, dst, index)
        loads[name].start()

    barrier = pltpu.get_barrier_semaphore()
    partners = set(range(1, group)) | {2**level for level in range(levels)}
    partners.add(2**last + 2 ** (last - 1))
    partners = sorted(partners)
    for mask in partners:
        pl.semaphore_signal(
            barrier, inc=1, device_id=device(mask), device_id_type=pl.DeviceIdType.MESH
        )

    def remote(src, dst, sends, recvs, index, mask, started):
        copy = pltpu.make_async_remote_copy(
            src_ref=src,
            dst_ref=dst,
            send_sem=sends.at[index],
            recv_sem=recvs.at[index],
            device_id=device(mask),
            device_id_type=pl.DeviceIdType.MESH,
        )
        copy.start()
        started.append(copy)
        return copy

    share = pl.ds(pl.multiple_of(leaf % 2 * (rank // 2), rank // 2), rank // 2)

    def block(i, n=1):
        return pl.ds(i * rank, n * rank)

    def factor(s, level, which):
        return local[s, root, which] if level == 0 else upper[s, level - 1, which]


    def chain(s, which):
        product = upper[s, bits - 2, which].astype(F32)
        for index in range(bits - 3, -1, -1):
            product = fold_cols(dot(upper[s, index, which], wide(product)))
        node = {root: fold_cols(dot(local[s, root, which], wide(product)))}
        for n in range(root - 1, -1, -1):
            parent = leaves + n // 2
            node[n] = fold_cols(dot(local[s, n, which], wide(node[parent])))
        return [node[i] for i in range(leaves)]

    def setup_chain(s):
        loads["local", s].wait()
        loads["upper", s].wait()
        et[...] = tall(lanes_of([v.T for v in chain(s, 0)]))

    def setup_up(s):
        loads["bases", s].wait()
        for i in range(leaves):
            vt[s, i] = bases[s, i, 1].astype(F32).T.astype(BF16)

    def setup_pairs(s):
        for p in range(leaves - 1):
            pair = [local[s, 2 * p + j, 0].astype(F32).T.astype(BF16) for j in range(2)]
            pt[p] = lanes_of(pair)

    def setup_couplings(s):
        loads["top", s].wait()
        for first, stop in ((1, bits), (bits, levels)):
            product = None
            for level in range(first, stop):
                coupling = top[s, top_pos] if level == last else upper[s, level - 1, 2]
                if product is None:
                    value = coupling.astype(F32)
                else:
                    value = fold_rows(dot(tall(product), coupling))
                tt[level] = wide(value.T)
                if level + 1 < stop:
                    q = upper[s, level - 1, 1]
                    product = q.astype(F32) if product is None else fold_rows(dot(tall(product), q))

    def setup_down(s):
        jt[...] = tall(rows_of(chain(s, 1)))

    def apply_first(prepare, hooks):
        s = 1
        started = []
        hooks = list(hooks)

        def start(src, dst, mask):
            return remote(src, dst, send_sem, recv_sem.at[1], len(started), mask, started)

        def across(value, level):
            return combine(dot(tall(value), tt[level]))

        def near_leaf(i):
            x_ref[i] = dot(near[s, i], r_ref[i].astype(BF16))

        def couple(n):
            sibling = n + 1 - 2 * (n % 2)
            pre[n] = fold_cols(dot(local[s, n, 2], cb[sibling]))

        field = {}

        def inner():
            for p in range(leaves - 1):
                stacked = rows_of([cb[2 * p], cb[2 * p + 1]])
                coefficient = fold_cols(dot(pt[p], stacked))
                if p < leaves - 2:
                    cb[leaves + p] = wide(coefficient)
            full[...] = fold_rows(dot(tall(coefficient.T), local[s, root, 0]))
            sib_full[0] = coefficient
            copy_a = start(full.at[pl.ds(other, half)], recv_a.at[0], 1)
            copies_b = [start(sib_full.at[0], sib_full.at[1], 1)]
            yield
            for level in range(1, bits):
                copy_a.wait_recv()
                if level == 1:
                    value = full[pl.ds(mine, half)] + recv_a[0]
                else:
                    value = send_a[level - 1] + recv_a[level - 1]
                if level < bits - 1:
                    send_a[level] = fold_rows(dot(tall(value), upper[s, level - 1, 0]))
                    copy_a = start(send_a.at[level], recv_a.at[level], 2**level)
                send_b[level] = value
                copies_b.append(start(send_b.at[level], recv_b.at[level], 2**level))
                if level == 1:
                    for n in range(root):
                        couple(n)
                    copies_b[0].wait_recv()
                    root_pre = fold_cols(dot(local[s, root, 2], wide(sib_full[1])))
                yield
            far = None
            for level in range(1, bits):
                copies_b[level].wait_recv()
                term = across(recv_b[level], level)
                far = term if far is None else far + term
            sib_full[2, pl.ds(mine, half)] = far
            piece = sib_full.at[2, pl.ds(mine, half)]
            copy = start(piece, piece, 1)
            yield
            copy.wait_recv()
            product = dot_nt(local[s, root, 1], tall(sib_full[2]))
            field[root] = fold_cols(product) + root_pre
            for n in range(root - 1, -1, -1):
                parent = leaves + n // 2
                field[n] = fold_cols(dot(local[s, n, 1], wide(field[parent]))) + pre[n]
            yield

        for i in range(leaves):
            cb[i] = wide(dot(vt[s, i], r_ref[i].astype(BF16)))
        stacked = rows_of([cb[i] for i in range(leaves)])
        outer_t = combine(dot(et[...], stacked)).T
        for j in range(group):
            w_send[j] = outer_t[j * cut : (j + 1) * cut]
        prepare()
        copies_w = []
        for e in range(group - 1, 0, -1):
            copies_w.append(start(w_send.at[member(device(e))], w_recv.at[e], e))
        steps = inner()
        work = list(range(leaves))

        def fill(everything=False):
            if hooks:
                hooks.pop(0)()
            next(steps, None)
            while work:
                near_leaf(work.pop(0))
                if not everything:
                    break

        fill()
        fill()
        for copy in copies_w:
            copy.wait_recv()
        value = w_send[me]
        for e in range(1, group):
            value = value + w_recv[e]
        far = None
        for level in range(bits, last - 1):
            high_a[level] = fold_rows(dot(tall(value), upper[s, level - 1, 0]))
            high_a[levels + level] = value
            copy_a = start(high_a.at[level], got_a.at[level], 2**level)
            copy_b = start(high_a.at[levels + level], got_a.at[levels + 1 + level], 2**level)
            fill()
            copy_a.wait_recv()
            value = high_a[level] + got_a[level]
            copy_b.wait_recv()
            term = across(got_a[levels + 1 + level], level)
            far = term if far is None else far + term
        low, high = last - 1, last
        high_a[high] = fold_rows(dot(tall(value), upper[s, low - 1, 0]))
        high_a[low] = value
        copies_top = [
            start(high_a.at[src], got_a.at[dst], mask)
            for src, dst, mask in (
                (high, high + 1, 2**high + 2**low),
                (high, high, 2**high),
                (low, low, 2**low),
            )
        ]
        fill()
        copies_top[2].wait_recv()
        term = across(got_a[low], low)
        far = term if far is None else far + term
        fill(True)
        copies_top[1].wait_recv()
        copies_top[0].wait_recv()
        far = far + across(got_a[high] + got_a[high + 1], high)
        plane[pl.ds(my_rows, cut)] = far
        copies_f = []
        for e in range(group - 1, 0, -1):
            piece = plane.at[pl.ds(my_rows, cut)]
            copies_f.append(start(piece, piece, e))
        for _ in steps:
            pass
        while hooks:
            hooks.pop(0)()
        for copy in copies_f:
            copy.wait_recv()
        outer = combine(dot_nt(jt[...], tall(plane[...])))
        for i in range(leaves):
            total = field[i] + outer[i * rank : (i + 1) * rank]
            value = x_ref[i] + dot(bases[s, i, 0], total.astype(BF16))
            x_ref[i] = value
            xw[i] = wide(value)
        for copy in started:
            copy.wait_send()


    pending = []
    own_part = {}
    replies = {}

    def local_chain(s, which):
        node = {}
        for n in range(root - 1, -1, -1):
            parent = leaves + n // 2
            own = local[s, n, which]
            if parent == root:
                node[n] = own.astype(F32)
            else:
                node[n] = fold_cols(dot(own, wide(node[parent])))
        return rows_of([node[i] for i in range(leaves)])

    def send_response(level, value):
        if value is not None:
            resp_send[level] = value
        replies["response", level] = remote(
            resp_send.at[level], resp_recv.at[level], fsend_sem, frecv_sem,
            levels + level, 2**level, pending,
        )

    def lift_response(level):
        own = fold_rows(dot(tall(resp_send[level]), factor(0, level, 1)))
        up = fac_send[level, :, :rank].astype(BF16)
        own_part[level] = fold_cols(dot(up, wide(own)))

    def prepare_response():
        loads["local", 0].wait()
        loads["upper", 0].wait()
        setup_up(0)
        for s in range(2):
            for which in range(2):
                chains[s, which] = local_chain(s, which)
        for i in range(leaves):
            gram[block(i)] = dot(vt[1, i], bases[0, i, 0])
        middle = rows_of([mm(gram[block(i)], chains[0, 1, block(i)]) for i in range(leaves)])
        resp_send[0] = -mm(chains[1, 0].T, middle)
        for level in range(last):
            fac_send[level] = lanes_of(
                [
                    factor(1, level, 0).astype(F32).T,
                    factor(0, level, 1).astype(F32),
                    factor(0, level, 2).astype(F32),
                ]
            )

    def send_factors():
        for level in range(last):
            part = pl.ds(0, rank) if level == 0 else share
            replies["factor", level] = remote(
                fac_send.at[level, part], fac_recv.at[level, part], fsend_sem, frecv_sem,
                level, 2**level, pending,
            )

    def forward_factor(level):
        replies["factor", level].wait_recv()
        piece = fac_recv.at[level, share]
        replies["factor", level] = remote(
            piece, piece, fsend_sem, frecv_sem, 2 * levels + level, 1, pending
        )

    def pack(level, x, y, d, c0, c1):
        zero = jnp.zeros((rank, rank), F32)
        if x is not None:
            p = [factor(s, level, 0).astype(F32) for s in range(2)]
            q = [factor(s, level, 1).astype(F32).T for s in range(2)]
            up_mat[level] = rows_of([lanes_of([p[0], x.T]), lanes_of([zero, p[1]])])
            down_mat[level] = rows_of([lanes_of([q[0], y.T]), lanes_of([zero, q[1]])])
            lift[level] = wide(up_mat[level])
        side_mat[level] = rows_of(
            [lanes_of([c0.astype(F32).T, zero]), lanes_of([zero, c1.astype(F32).T]), lanes_of([zero, d.T])]
        )

    def chain_step(level):
        replies["response", level].wait_recv()
        theirs = resp_recv[level]
        if level == last:
            u = fold_rows(dot(tall(theirs), top[0, 1 - top_pos]))
            c1 = top[1, top_pos]
            pack(level, None, None, fold_cols(dot(c1, wide(u))), top[0, top_pos], c1)
            return
        replies["factor", level].wait_recv()
        up = fac_recv[level, :, :rank].astype(BF16)
        sides = fac_recv[level, :, rank:].astype(BF16)
        mixed = fold_rows(dot(tall(theirs), sides))
        lifted = fold_cols(dot(up, wide(mixed)))
        send_response(level + 1, own_part[level] + lifted[:, :rank])
        if level + 1 < last:
            lift_response(level + 1)
        c1 = factor(1, level, 2)
        crossed = fold_cols(dot(c1, wide(mixed)))
        pack(
            level, lifted[:, rank:], crossed[:, :rank], crossed[:, rank:], factor(0, level, 2), c1
        )

    def setup_cross(first, stop):
        product = None
        for level in range(first, stop):
            value = side_mat[level]
            cross[level] = wide(value if product is None else mm(value, product))
            if level + 1 < stop or first == 1:
                step = down_mat[level]
                product = step if product is None else mm(step, product)
        return product

    def ancestors(i, j):
        while i // 2 != j // 2:
            i, j = leaves + i // 2, leaves + j // 2
        return i, j

    def partial(s, which, i, stop):
        value = local[s, i, which].astype(F32)
        n = leaves + i // 2
        while n != stop:
            value = fold_rows(dot(tall(value), local[s, n, which]))
            n = leaves + n // 2
        return value

    def setup_tree(s):
        size = leaves * rank
        tree[s] = jnp.zeros((2 * size, size), BF16)
        for i in range(leaves):
            for j in range(leaves):
                if i == j:
                    continue
                ni, nj = ancestors(i, j)
                if ni == i:
                    tree[s, block(i), block(j)] = local[s, i, 2]
                    continue
                down = fold_rows(dot(tall(partial(s, 1, i, ni)), local[s, ni, 2]))
                value = combine(dot_nt(tall(down), tall(partial(s, 0, j, nj))))
                hi, lo = split(value)
                tree[s, block(i), block(j)] = hi
                tree[s, pl.ds(size + i * rank, rank), block(j)] = lo

    def setup_near():
        loads["near", 0].wait()
        loads["rhs"].wait()
        for i in range(leaves):
            hi, lo = split(dot(vt[1, i], near[0, i]))
            near_coef[i] = rows_of([vt[0, i], hi, lo])
            rhs_coef[block(i)] = fold_cols(dot(vt[1, i], wide(b_ref[i])))

    def setup_base():
        size = leaves * rank
        inside = tree[0, :size].astype(F32) + tree[0, size:].astype(F32)
        mixed = rows_of([mm(gram[block(i)], inside[i * rank : (i + 1) * rank]) for i in range(leaves)])
        up0, up1 = chains[0, 0].T, chains[1, 0].T
        base_a[...] = rows_of([up0, -mm(up1, mixed)])
        base_b[...] = up1

    def setup_rise():
        up = up_mat[0].T
        for level in range(1, bits):
            up = mm(up_mat[level].T, up)
        out_a[...] = tall(mm(up, base_a[...]))
        out_b[...] = tall(mm(up[rank:, rank:], base_b[...]))

    def setup_enter():
        p0 = up_mat[0].T
        in_a[...] = tall(rows_of([base_a[...], mm(p0, base_a[...])]))
        in_b[...] = tall(rows_of([base_b[...], mm(p0[rank:, rank:], base_b[...])]))

    def setup_fall():
        down = setup_cross(1, bits)
        enter[...] = wide(rows_of([down_mat[0], side_mat[0]]))
        down = mm(down, down_mat[0])
        leaf_a[...] = tall(chains[0, 1])
        leaf_b[...] = tall(chains[1, 1])
        fall_a[...] = tall(combine(dot_nt(tall(chains[0, 1]), tall(down[:rank, :rank]))))
        fall_b[...] = tall(combine(dot_nt(tall(chains[1, 1]), tall(down[:, rank:]))))


    def merged(k, hooks):
        par = k % 2
        started = []
        hooks = list(hooks)

        def hook():
            if hooks:
                hooks.pop(0)()

        def start(src, dst, mask):
            return remote(
                src, dst, send_sem, recv_sem.at[par], len(started), mask, started
            )

        def across(level, sibling, own):
            value = lanes_of([sibling, own[:, :rank]])
            return combine(dot(tall(value), cross[level]))

        for i in range(leaves):
            out = dot(near_coef[i], xw[i])
            a = fold_cols(out[:rank])
            near_part = out[rank : 2 * rank, :columns] + (
                out[rank : 2 * rank, columns:] + out[2 * rank :, :columns]
            )
            stack[0, block(i)] = wide(a)
            stack[1, block(i)] = wide(rhs_coef[block(i)] - near_part)
        outer = combine(dot(out_a[...], stack[0]))
        outer_b = outer[rank:] + combine(dot(out_b[...], stack[1]))
        outer_t = lanes_of([outer[:rank].T, outer_b.T])
        for j in range(group):
            jw_send[par, j] = outer_t[j * cut : (j + 1) * cut]
        copies_w = []
        for e in range(group - 1, 0, -1):
            copies_w.append(start(jw_send.at[par, member(device(e))], jw_recv.at[par, e], e))

        hook()

        def inner():
            wide_in = combine(dot(in_a[...], stack[0]))
            narrow = combine(dot(in_b[...], stack[1]))
            jsib[par, 0] = lanes_of([wide_in[:rank].T, (wide_in[rank : 2 * rank] + narrow[:rank]).T])
            jfull[par] = lanes_of(
                [wide_in[2 * rank : 3 * rank].T, (wide_in[3 * rank :] + narrow[rank:]).T]
            )
            copy_a = start(jfull.at[par, pl.ds(other, half)], jr_a.at[par, 0], 1)
            copies_b = [start(jsib.at[par, 0], jsib.at[par, 1], 1)]
            yield
            for level in range(1, bits):
                copy_a.wait_recv()
                if level == 1:
                    value = jfull[par, pl.ds(mine, half)] + jr_a[par, 0]
                else:
                    value = js_a[par, level - 1] + jr_a[par, level - 1]
                if level < bits - 1:
                    js_a[par, level] = combine(dot(tall(value), lift[level]))
                    copy_a = start(js_a.at[par, level], jr_a.at[par, level], 2**level)
                js_b[par, level] = value
                copies_b.append(start(js_b.at[par, level], jr_b.at[par, level], 2**level))
                yield
            far = None
            for level in range(1, bits):
                copies_b[level].wait_recv()
                term = across(level, jr_b[par, level], js_b[par, level])
                far = term if far is None else far + term
            jsib[par, 2, pl.ds(mine, half)] = far
            piece = jsib.at[par, 2, pl.ds(mine, half)]
            copy = start(piece, piece, 1)
            yield
            copies_b[0].wait_recv()
            copy.wait_recv()
            value = lanes_of([jsib[par, 2], jsib[par, 1], jsib[par, 0, :, :rank]])
            value = combine(dot(tall(value), enter[...]))
            field_a[...] = combine(dot_nt(leaf_a[...], tall(value[:, :rank])))
            field_b[...] = combine(dot_nt(leaf_b[...], tall(value[:, rank:])))
            yield

        steps = inner()
        next(steps)
        inside = combine(dot(tree[0], stack[0]))

        def residual(i):
            part = fold_cols(dot(bases[0, i, 0], wide(inside[i * rank : (i + 1) * rank])))
            r_ref[i] = b_ref[i] - fold_cols(dot(near[0, i], xw[i])) - part

        residual(0)
        next(steps)
        hook()
        for i in range(1, leaves):
            residual(i)
        for copy in copies_w:
            copy.wait_recv()
        value = jw_send[par, me]
        for e in range(1, group):
            value = value + jw_recv[par, e]
        far = None
        for level in range(bits, last - 1):
            jhigh[par, level] = combine(dot(tall(value), lift[level]))
            jhigh[par, levels + level] = value
            copy_a = start(jhigh.at[par, level], jgot.at[par, level], 2**level)
            copy_b = start(
                jhigh.at[par, levels + level], jgot.at[par, levels + 2 + level], 2**level
            )
            copy_a.wait_recv()
            copy_b.wait_recv()
            term = across(level, jgot[par, levels + 2 + level], value)
            far = term if far is None else far + term
            value = jhigh[par, level] + jgot[par, level]
        low, high = last - 1, last
        jhigh[par, high] = combine(dot(tall(value), lift[low]))
        jhigh[par, low] = value
        copies_top = [
            start(jhigh.at[par, src], jgot.at[par, dst], mask)
            for src, dst, mask in (
                (high, high + 1, 2**high + 2**low),
                (high, high, 2**high),
                (high, high + 2, 2**low),
                (low, low, 2**low),
            )
        ]
        for _ in range(bits - 2):
            next(steps)
        hook()
        copies_top[3].wait_recv()
        term = across(low, jgot[par, low], value)
        far = term if far is None else far + term
        for copy in copies_top[:3]:
            copy.wait_recv()
        own = jhigh[par, high] + jgot[par, high + 2]
        far = far + across(high, jgot[par, high] + jgot[par, high + 1], own)
        jplane[par, pl.ds(my_rows, cut)] = far
        copies_f = []
        for e in range(group - 1, 0, -1):
            piece = jplane.at[par, pl.ds(my_rows, cut)]
            copies_f.append(start(piece, piece, e))
        for _ in steps:
            pass
        for copy in copies_f:
            copy.wait_recv()
        flat = tall(jplane[par])
        alpha = field_a[...] + combine(dot_nt(fall_a[...], flat[:, :rank]))
        sums = None
        for i in range(leaves):
            out = r_ref[i] - fold_cols(dot(bases[0, i, 0], wide(alpha[i * rank : (i + 1) * rank])))
            low_out = out.astype(BF16)
            rb[i] = low_out
            stack[0, block(i)] = wide(dot(vt[1, i], low_out))
            square = jnp.sum((out * out).reshape(-1, 8, columns), axis=0)
            sums = square if sums is None else sums + square
        nrm[pl.ds(k, 1)] = jnp.sum(sums, axis=0, keepdims=True)
        if k == STEPS - 1:
            start_norms()
        beta = field_b[...] + combine(dot_nt(fall_b[...], flat))
        beta = beta + combine(dot(tree[1], stack[0]))
        for i in range(leaves):
            far = beta[i * rank : (i + 1) * rank].astype(BF16)
            value = x_ref[i] + (dot(near[1, i], rb[i]) + dot(bases[1, i, 0], far))
            x_ref[i] = value
            if k < STEPS - 1:
                xw[i] = wide(value)
        for copy in started:
            copy.wait_send()

    def norm_round(index, value):
        lo, hi = norm_rounds(levels)[index]
        nsend[index, pl.ds(0, STEPS)] = value
        for m in range(2 ** (hi - lo) - 1, 0, -1):
            pltpu.make_async_remote_copy(
                src_ref=nsend.at[index, pl.ds(0, STEPS)],
                dst_ref=nrecv.at[index, m, pl.ds(0, STEPS)],
                send_sem=nsend_sem.at[index],
                recv_sem=nrecv_sem.at[index],
                device_id=device(m << lo),
                device_id_type=pl.DeviceIdType.MESH,
            ).start()

    def start_norms():
        norm_round(0, nrm[pl.ds(0, STEPS)])

    def finish_norms():
        waits = []
        for index, (lo, hi) in enumerate(norm_rounds(levels)):
            if index:
                norm_round(index, value)
            count = 2 ** (hi - lo)
            every = nrecv.at[index, pl.ds(1, count - 1), pl.ds(0, STEPS)]
            pltpu.make_async_copy(every, every, nrecv_sem.at[index]).wait()
            waits.append(pltpu.make_async_copy(every, every, nsend_sem.at[index]))
            value = nsend[index, pl.ds(0, STEPS)]
            for m in range(1, count):
                value = value + nrecv[index, m, pl.ds(0, STEPS)]
        norm_ref[...] = value
        for copy in waits:
            copy.wait()

    setup_chain(1)
    setup_up(1)
    loads["res"].wait()

    def prepare():
        prepare_response()
        setup_tree(0)
        pl.semaphore_wait(barrier, len(partners))

    def first():
        send_response(0, None)
        send_factors()
        lift_response(0)
        setup_pairs(1)
        loads["near", 1].wait()

    def second():
        chain_step(0)
        setup_couplings(1)
        setup_down(1)

    def third():
        for level in range(1, bits):
            forward_factor(level)
        loads["top", 0].wait()
        setup_near()
        chain_step(1)

    def fourth():
        setup_base()
        setup_tree(1)

    def fifth():
        for level in range(bits, last):
            forward_factor(level)
        for level in range(2, bits):
            chain_step(level)
        setup_rise()

    def sixth():
        setup_enter()
        for level in range(bits, last):
            chain_step(level)

    def eighth():
        chain_step(last)
        setup_cross(bits, levels)
        for copy in pending:
            copy.wait_send()

    apply_first(prepare, [first, second, third, fourth, fifth])
    merged(0, [sixth, setup_fall, eighth])
    for k in range(1, STEPS):
        merged(k, [lambda: None])
    finish_norms()


def body(right_sides, near_blocks, leaf_bases, local_factors, upper_factors, top_couplings):
    bits_leaf = lax.axis_size("leaf").bit_length() - 1
    bits_rows = lax.axis_size("rows").bit_length() - 1
    levels = bits_leaf + bits_rows
    leaves, size = near_blocks.shape[1], near_blocks.shape[2]
    rank = leaf_bases.shape[4]
    columns = right_sides.shape[1]
    half = columns // 2
    bits = group_bits(levels)
    group = 2**bits
    cut = columns // group
    copies = 2 * (group - 1) + 2 * bits + 2 * (levels - 2 - bits) + 4
    nodes = local_factors.shape[1]
    heights = upper_factors.shape[2]
    flat = leaves * rank
    pair = 2 * rank
    rounds = len(norm_rounds(levels))
    vmem = pltpu.VMEM
    dma = pltpu.SemaphoreType.DMA
    out, norms = pl.pallas_call(
        functools.partial(kernel, bits_leaf, bits_rows),
        out_shape=(
            vmem((leaves, size, columns), F32),
            vmem((STEPS, columns), F32),
        ),
        in_specs=[pl.BlockSpec(memory_space=pl.ANY)] * 6,
        out_specs=(pl.BlockSpec(memory_space=vmem), pl.BlockSpec(memory_space=vmem)),
        scratch_shapes=[
            vmem((leaves, size, columns), F32),
            vmem((leaves, size, columns), F32),
            vmem((2, leaves, size, size), BF16),
            vmem((2, leaves, 2, size, rank), BF16),
            vmem((2, nodes, 3, rank, rank), BF16),
            vmem((2, heights, 3, rank, rank), BF16),
            vmem((2, 2, rank, rank), BF16),
            vmem((2, leaves, rank, size), BF16),
            vmem((leaves - 1, rank, 2 * rank), BF16),
            vmem((levels, rank, 2 * rank), BF16),
            vmem((2 * rank, leaves * rank), BF16),
            vmem((2 * leaves * rank, rank), BF16),
            vmem((nodes - 1, rank, 2 * columns), BF16),
            vmem((nodes - 1, rank, columns), F32),
            vmem((8, columns), F32),
            vmem((group, cut, rank), F32),
            vmem((group, cut, rank), F32),
            vmem((2 * levels, cut, rank), F32),
            vmem((2 * levels + 1, cut, rank), F32),
            vmem((columns, rank), F32),
            vmem((bits, half, rank), F32),
            vmem((bits, half, rank), F32),
            vmem((bits, half, rank), F32),
            vmem((bits, half, rank), F32),
            vmem((3, rank, columns), F32),
            vmem((columns, rank), F32),
            vmem((levels - 1, rank, 3 * rank), F32),
            vmem((levels - 1, rank, 3 * rank), F32),
            vmem((levels, rank, rank), F32),
            vmem((levels, rank, rank), F32),
            vmem((levels, pair, pair), F32),
            vmem((levels, pair, pair), F32),
            vmem((levels, 3 * rank, pair), F32),
            vmem((flat, rank), F32),
            vmem((pair, flat), F32),
            vmem((rank, flat), F32),
            vmem((2, 2, flat, rank), F32),
            vmem((leaves, 3 * rank, size), BF16),
            vmem((flat, columns), F32),
            vmem((2, 2 * flat, flat), BF16),
            vmem((2, flat, 2 * columns), BF16),
            vmem((2 * pair, flat), BF16),
            vmem((pair, flat), BF16),
            vmem((4 * pair, flat), BF16),
            vmem((2 * pair, flat), BF16),
            vmem((levels, pair, 2 * pair), BF16),
            vmem((levels, 3 * rank, 2 * pair), BF16),
            vmem((5 * rank, 2 * pair), BF16),
            vmem((2 * flat, rank), BF16),
            vmem((2 * flat, pair), BF16),
            vmem((2 * flat, rank), BF16),
            vmem((2 * flat, rank), BF16),
            vmem((leaves, size, 2 * columns), BF16),
            vmem((leaves, size, columns), BF16),
            vmem((flat, columns), F32),
            vmem((flat, columns), F32),
            vmem((2, group, cut, pair), F32),
            vmem((2, group, cut, pair), F32),
            vmem((2, 2 * levels, cut, pair), F32),
            vmem((2, 2 * levels + 2, cut, pair), F32),
            vmem((2, columns, pair), F32),
            vmem((2, bits, half, pair), F32),
            vmem((2, bits, half, pair), F32),
            vmem((2, bits, half, pair), F32),
            vmem((2, bits, half, pair), F32),
            vmem((2, 3, columns, pair), F32),
            vmem((2, columns, pair), F32),
            vmem((rounds, 8, columns), F32),
            vmem((rounds, 32, 8, columns), F32),
            dma((12,)),
            dma((copies,)),
            dma((2, copies)),
            dma((3 * levels,)),
            dma((3 * levels,)),
            dma((rounds,)),
            dma((rounds,)),
        ],
        compiler_params=pltpu.CompilerParams(
            collective_id=0, has_side_effects=True, vmem_limit_bytes=60000000
        ),
    )(
        right_sides.reshape(leaves, size, columns),
        near_blocks,
        leaf_bases,
        local_factors,
        upper_factors,
        top_couplings,
    )
    return out.reshape(-1, columns), norms


def solution(mesh):
    placed = (
        P(("rows", "leaf"), None),
        P(None, ("rows", "leaf"), None, None),
        P(None, ("rows", "leaf"), None, None, None),
        P(None, ("rows", "leaf"), None, None, None),
        P(None, ("rows", "leaf"), None, None, None, None),
        P(),
    )
    return jax.shard_map(
        body,
        mesh=mesh,
        in_specs=placed,
        out_specs=(P(("rows", "leaf"), None), P()),
        check_vma=False,
    )
```

```python
import functools
import jax
import jax.numpy as jnp
from jax import lax
from jax.experimental import pallas as pl
from jax.experimental.pallas import tpu as pltpu
from jax.sharding import PartitionSpec as P

STEPS = 3
F32 = jnp.float32
BF16 = jnp.bfloat16
NT = (((1,), (1,)), ((), ()))


def dot(a, b):
    return jnp.dot(a, b, preferred_element_type=F32)


def split(v):
    hi = v.astype(BF16)
    lo = (v - hi.astype(F32)).astype(BF16)
    return hi, lo


def wide(v):
    return jnp.concatenate(split(v), axis=1)


def tall(v):
    return jnp.concatenate(split(v), axis=0)


def fold_cols(v):
    n = v.shape[1] // 2
    return v[:, :n] + v[:, n:]


def fold_rows(v):
    n = v.shape[0] // 2
    return v[:n] + v[n:]


def combine(out):
    n, m = out.shape[0] // 2, out.shape[1] // 2
    return out[:n, :m] + (out[:n, m:] + out[n:, :m])


def mm(a, b):
    return combine(dot(tall(a), wide(b)))


def dot_nt(a, b):
    return lax.dot_general(a, b, NT, preferred_element_type=F32)


def rows_of(parts):
    return jnp.concatenate(parts, axis=0)


def lanes_of(parts):
    return jnp.concatenate(parts, axis=1)


def norm_rounds(levels):
    return [(lo, min(lo + 5, levels)) for lo in range(0, levels, 5)]


def group_bits(levels):
    return min(3, levels - 2)


def kernel(
    bits_leaf, bits_rows,
    rhs_hbm, near_hbm, bases_hbm, local_hbm, upper_hbm, top_hbm,
    x_ref, norm_ref,
    b_ref, r_ref, near, bases, local, upper, top,
    vt, pt, tt, et, jt, cb, pre, nrm,
    w_send, w_recv, high_a, got_a, plane,
    send_a, send_b, recv_a, recv_b, sib_full, full,
    fac_send, fac_recv, resp_send, resp_recv,
    up_mat, down_mat, side_mat,
    gram, base_a, base_b,
    chains, near_coef, rhs_coef, tree, stack,
    out_a, out_b, in_a, in_b, lift, cross, enter,
    fall_a, fall_b, leaf_a, leaf_b, xw, rb, field_a, field_b,
    jw_send, jw_recv, jhigh, jgot, jplane,
    js_a, js_b, jr_a, jr_b, jsib, jfull,
    nsend, nrecv,
    load_sem, send_sem, recv_sem, fsend_sem, frecv_sem, nsend_sem, nrecv_sem,
):
    leaves = near.shape[1]
    levels = bits_leaf + bits_rows
    last = levels - 1
    bits = group_bits(levels)
    group = 2**bits
    root = 2 * leaves - 2
    leaf = lax.axis_index("leaf")
    rows = lax.axis_index("rows")
    columns = x_ref.shape[2]
    rank = plane.shape[1]
    half = columns // 2
    cut = columns // group
    mine = pl.multiple_of(leaf % 2 * half, half)
    other = pl.multiple_of((1 - leaf % 2) * half, half)
    top_pos = rows // 2 ** (bits_rows - 1)

    def flipped(value, mask):
        for bit in range(mask.bit_length()):
            d = 2**bit
            if mask & d:
                value = value + d - 2 * d * (value // d % 2)
        return value

    def device(mask):
        leaf_mask = mask % 2**bits_leaf
        return (flipped(rows, mask // 2**bits_leaf), flipped(leaf, leaf_mask))

    def member(place):
        row, column = place
        if bits <= bits_leaf:
            return column % group
        return column + 2**bits_leaf * (row % 2 ** (bits - bits_leaf))

    me = member((rows, leaf))
    my_rows = pl.multiple_of(me * cut, cut)

    def load(src, dst, index):
        return pltpu.make_async_copy(src, dst, load_sem.at[index])

    loads = {}
    order = []
    for s in (1, 0):
        order += [
            (("local", s), local_hbm.at[s], local.at[s]),
            (("upper", s), upper_hbm.at[s, 0], upper.at[s]),
            (("bases", s), bases_hbm.at[s], bases.at[s]),
        ]
        if s == 1:
            order += [("res", rhs_hbm, r_ref)]
        order += [
            (("near", s), near_hbm.at[s], near.at[s]),
            (("top", s), top_hbm.at[s], top.at[s]),
        ]
        if s == 1:
            order += [("rhs", rhs_hbm, b_ref)]
    for index, (name, src, dst) in enumerate(order):
        loads[name] = load(src, dst, index)
        loads[name].start()

    barrier = pltpu.get_barrier_semaphore()
    partners = set(range(1, group)) | {2**level for level in range(levels)}
    partners.add(2**last + 2 ** (last - 1))
    partners = sorted(partners)
    for mask in partners:
        pl.semaphore_signal(
            barrier, inc=1, device_id=device(mask), device_id_type=pl.DeviceIdType.MESH
        )

    def remote(src, dst, sends, recvs, index, mask, started):
        copy = pltpu.make_async_remote_copy(
            src_ref=src,
            dst_ref=dst,
            send_sem=sends.at[index],
            recv_sem=recvs.at[index],
            device_id=device(mask),
            device_id_type=pl.DeviceIdType.MESH,
        )
        copy.start()
        started.append(copy)
        return copy

    share = pl.ds(pl.multiple_of(leaf % 2 * (rank // 2), rank // 2), rank // 2)

    def block(i, n=1):
        return pl.ds(i * rank, n * rank)

    def factor(s, level, which):
        return local[s, root, which] if level == 0 else upper[s, level - 1, which]


    def chain(s, which):
        product = upper[s, bits - 2, which].astype(F32)
        for index in range(bits - 3, -1, -1):
            product = fold_cols(dot(upper[s, index, which], wide(product)))
        node = {root: fold_cols(dot(local[s, root, which], wide(product)))}
        for n in range(root - 1, -1, -1):
            parent = leaves + n // 2
            node[n] = fold_cols(dot(local[s, n, which], wide(node[parent])))
        return [node[i] for i in range(leaves)]

    def setup_chain(s):
        loads["local", s].wait()
        loads["upper", s].wait()
        et[...] = tall(lanes_of([v.T for v in chain(s, 0)]))

    def setup_up(s):
        loads["bases", s].wait()
        for i in range(leaves):
            vt[s, i] = bases[s, i, 1].astype(F32).T.astype(BF16)

    def setup_pairs(s):
        for p in range(leaves - 1):
            pair = [local[s, 2 * p + j, 0].astype(F32).T.astype(BF16) for j in range(2)]
            pt[p] = lanes_of(pair)

    def setup_couplings(s):
        loads["top", s].wait()
        for first, stop in ((1, bits), (bits, levels)):
            product = None
            for level in range(first, stop):
                coupling = top[s, top_pos] if level == last else upper[s, level - 1, 2]
                if product is None:
                    value = coupling.astype(F32)
                else:
                    value = fold_rows(dot(tall(product), coupling))
                tt[level] = wide(value.T)
                if level + 1 < stop:
                    q = upper[s, level - 1, 1]
                    product = q.astype(F32) if product is None else fold_rows(dot(tall(product), q))

    def setup_down(s):
        jt[...] = tall(rows_of(chain(s, 1)))

    def apply_first(prepare, hooks):
        s = 1
        started = []
        hooks = list(hooks)

        def start(src, dst, mask):
            return remote(src, dst, send_sem, recv_sem.at[1], len(started), mask, started)

        def across(value, level):
            return combine(dot(tall(value), tt[level]))

        def near_leaf(i):
            x_ref[i] = dot(near[s, i], r_ref[i].astype(BF16))

        def couple(n):
            sibling = n + 1 - 2 * (n % 2)
            pre[n] = fold_cols(dot(local[s, n, 2], cb[sibling]))

        field = {}

        def inner():
            for p in range(leaves - 1):
                stacked = rows_of([cb[2 * p], cb[2 * p + 1]])
                coefficient = fold_cols(dot(pt[p], stacked))
                if p < leaves - 2:
                    cb[leaves + p] = wide(coefficient)
            full[...] = fold_rows(dot(tall(coefficient.T), local[s, root, 0]))
            sib_full[0] = coefficient
            copy_a = start(full.at[pl.ds(other, half)], recv_a.at[0], 1)
            copies_b = [start(sib_full.at[0], sib_full.at[1], 1)]
            yield
            for level in range(1, bits):
                copy_a.wait_recv()
                if level == 1:
                    value = full[pl.ds(mine, half)] + recv_a[0]
                else:
                    value = send_a[level - 1] + recv_a[level - 1]
                if level < bits - 1:
                    send_a[level] = fold_rows(dot(tall(value), upper[s, level - 1, 0]))
                    copy_a = start(send_a.at[level], recv_a.at[level], 2**level)
                send_b[level] = value
                copies_b.append(start(send_b.at[level], recv_b.at[level], 2**level))
                if level == 1:
                    for n in range(root):
                        couple(n)
                    copies_b[0].wait_recv()
                    root_pre = fold_cols(dot(local[s, root, 2], wide(sib_full[1])))
                yield
            far = None
            for level in range(1, bits):
                copies_b[level].wait_recv()
                term = across(recv_b[level], level)
                far = term if far is None else far + term
            sib_full[2, pl.ds(mine, half)] = far
            piece = sib_full.at[2, pl.ds(mine, half)]
            copy = start(piece, piece, 1)
            yield
            copy.wait_recv()
            product = dot_nt(local[s, root, 1], tall(sib_full[2]))
            field[root] = fold_cols(product) + root_pre
            for n in range(root - 1, -1, -1):
                parent = leaves + n // 2
                field[n] = fold_cols(dot(local[s, n, 1], wide(field[parent]))) + pre[n]
            yield

        for i in range(leaves):
            cb[i] = wide(dot(vt[s, i], r_ref[i].astype(BF16)))
        stacked = rows_of([cb[i] for i in range(leaves)])
        outer_t = combine(dot(et[...], stacked)).T
        for j in range(group):
            w_send[j] = outer_t[j * cut : (j + 1) * cut]
        prepare()
        copies_w = []
        for e in range(group - 1, 0, -1):
            copies_w.append(start(w_send.at[member(device(e))], w_recv.at[e], e))
        steps = inner()
        work = list(range(leaves))

        def fill(everything=False):
            if hooks:
                hooks.pop(0)()
            next(steps, None)
            while work:
                near_leaf(work.pop(0))
                if not everything:
                    break

        fill()
        fill()
        for copy in copies_w:
            copy.wait_recv()
        value = w_send[me]
        for e in range(1, group):
            value = value + w_recv[e]
        far = None
        for level in range(bits, last - 1):
            high_a[level] = fold_rows(dot(tall(value), upper[s, level - 1, 0]))
            high_a[levels + level] = value
            copy_a = start(high_a.at[level], got_a.at[level], 2**level)
            copy_b = start(high_a.at[levels + level], got_a.at[levels + 1 + level], 2**level)
            fill()
            copy_a.wait_recv()
            value = high_a[level] + got_a[level]
            copy_b.wait_recv()
            term = across(got_a[levels + 1 + level], level)
            far = term if far is None else far + term
        low, high = last - 1, last
        high_a[high] = fold_rows(dot(tall(value), upper[s, low - 1, 0]))
        high_a[low] = value
        copies_top = [
            start(high_a.at[src], got_a.at[dst], mask)
            for src, dst, mask in (
                (high, high + 1, 2**high + 2**low),
                (high, high, 2**high),
                (low, low, 2**low),
            )
        ]
        fill()
        copies_top[2].wait_recv()
        term = across(got_a[low], low)
        far = term if far is None else far + term
        fill(True)
        copies_top[1].wait_recv()
        copies_top[0].wait_recv()
        far = far + across(got_a[high] + got_a[high + 1], high)
        plane[pl.ds(my_rows, cut)] = far
        copies_f = []
        for e in range(group - 1, 0, -1):
            piece = plane.at[pl.ds(my_rows, cut)]
            copies_f.append(start(piece, piece, e))
        for _ in steps:
            pass
        while hooks:
            hooks.pop(0)()
        for copy in copies_f:
            copy.wait_recv()
        outer = combine(dot_nt(jt[...], tall(plane[...])))
        for i in range(leaves):
            total = field[i] + outer[i * rank : (i + 1) * rank]
            value = x_ref[i] + dot(bases[s, i, 0], total.astype(BF16))
            x_ref[i] = value
            xw[i] = wide(value)
        for copy in started:
            copy.wait_send()


    pending = []
    own_part = {}
    replies = {}

    def local_chain(s, which):
        node = {}
        for n in range(root - 1, -1, -1):
            parent = leaves + n // 2
            own = local[s, n, which]
            if parent == root:
                node[n] = own.astype(F32)
            else:
                node[n] = fold_cols(dot(own, wide(node[parent])))
        return rows_of([node[i] for i in range(leaves)])

    def send_response(level, value):
        if value is not None:
            resp_send[level] = value
        replies["response", level] = remote(
            resp_send.at[level], resp_recv.at[level], fsend_sem, frecv_sem,
            levels + level, 2**level, pending,
        )

    def lift_response(level):
        own = fold_rows(dot(tall(resp_send[level]), factor(0, level, 1)))
        up = fac_send[level, :, :rank].astype(BF16)
        own_part[level] = fold_cols(dot(up, wide(own)))

    def prepare_response():
        loads["local", 0].wait()
        loads["upper", 0].wait()
        setup_up(0)
        for s in range(2):
            for which in range(2):
                chains[s, which] = local_chain(s, which)
        for i in range(leaves):
            gram[block(i)] = dot(vt[1, i], bases[0, i, 0])
        middle = rows_of([mm(gram[block(i)], chains[0, 1, block(i)]) for i in range(leaves)])
        resp_send[0] = -mm(chains[1, 0].T, middle)
        for level in range(last):
            fac_send[level] = lanes_of(
                [
                    factor(1, level, 0).astype(F32).T,
                    factor(0, level, 1).astype(F32),
                    factor(0, level, 2).astype(F32),
                ]
            )

    def send_factors():
        for level in range(last):
            part = pl.ds(0, rank) if level == 0 else share
            replies["factor", level] = remote(
                fac_send.at[level, part], fac_recv.at[level, part], fsend_sem, frecv_sem,
                level, 2**level, pending,
            )

    def forward_factor(level):
        replies["factor", level].wait_recv()
        piece = fac_recv.at[level, share]
        replies["factor", level] = remote(
            piece, piece, fsend_sem, frecv_sem, 2 * levels + level, 1, pending
        )

    def pack(level, x, y, d, c0, c1):
        zero = jnp.zeros((rank, rank), F32)
        if x is not None:
            p = [factor(s, level, 0).astype(F32) for s in range(2)]
            q = [factor(s, level, 1).astype(F32).T for s in range(2)]
            up_mat[level] = rows_of([lanes_of([p[0], x.T]), lanes_of([zero, p[1]])])
            down_mat[level] = rows_of([lanes_of([q[0], y.T]), lanes_of([zero, q[1]])])
            lift[level] = wide(up_mat[level])
        side_mat[level] = rows_of(
            [lanes_of([c0.astype(F32).T, zero]), lanes_of([zero, c1.astype(F32).T]), lanes_of([zero, d.T])]
        )

    def chain_step(level):
        replies["response", level].wait_recv()
        theirs = resp_recv[level]
        if level == last:
            u = fold_rows(dot(tall(theirs), top[0, 1 - top_pos]))
            c1 = top[1, top_pos]
            pack(level, None, None, fold_cols(dot(c1, wide(u))), top[0, top_pos], c1)
            return
        replies["factor", level].wait_recv()
        up = fac_recv[level, :, :rank].astype(BF16)
        sides = fac_recv[level, :, rank:].astype(BF16)
        mixed = fold_rows(dot(tall(theirs), sides))
        lifted = fold_cols(dot(up, wide(mixed)))
        send_response(level + 1, own_part[level] + lifted[:, :rank])
        if level + 1 < last:
            lift_response(level + 1)
        c1 = factor(1, level, 2)
        crossed = fold_cols(dot(c1, wide(mixed)))
        pack(
            level, lifted[:, rank:], crossed[:, :rank], crossed[:, rank:], factor(0, level, 2), c1
        )

    def setup_cross(first, stop):
        product = None
        for level in range(first, stop):
            value = side_mat[level]
            cross[level] = wide(value if product is None else mm(value, product))
            if level + 1 < stop or first == 1:
                step = down_mat[level]
                product = step if product is None else mm(step, product)
        return product

    def ancestors(i, j):
        while i // 2 != j // 2:
            i, j = leaves + i // 2, leaves + j // 2
        return i, j

    def partial(s, which, i, stop):
        value = local[s, i, which].astype(F32)
        n = leaves + i // 2
        while n != stop:
            value = fold_rows(dot(tall(value), local[s, n, which]))
            n = leaves + n // 2
        return value

    def setup_tree(s):
        size = leaves * rank
        tree[s] = jnp.zeros((2 * size, size), BF16)
        for i in range(leaves):
            for j in range(leaves):
                if i == j:
                    continue
                ni, nj = ancestors(i, j)
                if ni == i:
                    tree[s, block(i), block(j)] = local[s, i, 2]
                    continue
                down = fold_rows(dot(tall(partial(s, 1, i, ni)), local[s, ni, 2]))
                value = combine(dot_nt(tall(down), tall(partial(s, 0, j, nj))))
                hi, lo = split(value)
                tree[s, block(i), block(j)] = hi
                tree[s, pl.ds(size + i * rank, rank), block(j)] = lo

    def setup_near():
        loads["near", 0].wait()
        loads["rhs"].wait()
        for i in range(leaves):
            hi, lo = split(dot(vt[1, i], near[0, i]))
            near_coef[i] = rows_of([vt[0, i], hi, lo])
            rhs_coef[block(i)] = fold_cols(dot(vt[1, i], wide(b_ref[i])))

    def setup_base():
        size = leaves * rank
        inside = tree[0, :size].astype(F32) + tree[0, size:].astype(F32)
        mixed = rows_of([mm(gram[block(i)], inside[i * rank : (i + 1) * rank]) for i in range(leaves)])
        up0, up1 = chains[0, 0].T, chains[1, 0].T
        base_a[...] = rows_of([up0, -mm(up1, mixed)])
        base_b[...] = up1

    def setup_rise():
        up = up_mat[0].T
        for level in range(1, bits):
            up = mm(up_mat[level].T, up)
        out_a[...] = tall(mm(up, base_a[...]))
        out_b[...] = tall(mm(up[rank:, rank:], base_b[...]))

    def setup_enter():
        p0 = up_mat[0].T
        in_a[...] = tall(rows_of([base_a[...], mm(p0, base_a[...])]))
        in_b[...] = tall(rows_of([base_b[...], mm(p0[rank:, rank:], base_b[...])]))

    def setup_fall():
        down = setup_cross(1, bits)
        enter[...] = wide(rows_of([down_mat[0], side_mat[0]]))
        down = mm(down, down_mat[0])
        leaf_a[...] = tall(chains[0, 1])
        leaf_b[...] = tall(chains[1, 1])
        fall_a[...] = tall(combine(dot_nt(tall(chains[0, 1]), tall(down[:rank, :rank]))))
        fall_b[...] = tall(combine(dot_nt(tall(chains[1, 1]), tall(down[:, rank:]))))


    def merged(k, hooks):
        par = k % 2
        started = []
        hooks = list(hooks)

        def hook():
            if hooks:
                hooks.pop(0)()

        def start(src, dst, mask):
            return remote(
                src, dst, send_sem, recv_sem.at[par], len(started), mask, started
            )

        def across(level, sibling, own):
            value = lanes_of([sibling, own[:, :rank]])
            return combine(dot(tall(value), cross[level]))

        for i in range(leaves):
            out = dot(near_coef[i], xw[i])
            a = fold_cols(out[:rank])
            near_part = out[rank : 2 * rank, :columns] + (
                out[rank : 2 * rank, columns:] + out[2 * rank :, :columns]
            )
            stack[0, block(i)] = wide(a)
            stack[1, block(i)] = wide(rhs_coef[block(i)] - near_part)
        outer = combine(dot(out_a[...], stack[0]))
        outer_b = outer[rank:] + combine(dot(out_b[...], stack[1]))
        outer_t = lanes_of([outer[:rank].T, outer_b.T])
        for j in range(group):
            jw_send[par, j] = outer_t[j * cut : (j + 1) * cut]
        copies_w = []
        for e in range(group - 1, 0, -1):
            copies_w.append(start(jw_send.at[par, member(device(e))], jw_recv.at[par, e], e))

        hook()

        def inner():
            wide_in = combine(dot(in_a[...], stack[0]))
            narrow = combine(dot(in_b[...], stack[1]))
            jsib[par, 0] = lanes_of([wide_in[:rank].T, (wide_in[rank : 2 * rank] + narrow[:rank]).T])
            jfull[par] = lanes_of(
                [wide_in[2 * rank : 3 * rank].T, (wide_in[3 * rank :] + narrow[rank:]).T]
            )
            copy_a = start(jfull.at[par, pl.ds(other, half)], jr_a.at[par, 0], 1)
            copies_b = [start(jsib.at[par, 0], jsib.at[par, 1], 1)]
            yield
            for level in range(1, bits):
                copy_a.wait_recv()
                if level == 1:
                    value = jfull[par, pl.ds(mine, half)] + jr_a[par, 0]
                else:
                    value = js_a[par, level - 1] + jr_a[par, level - 1]
                if level < bits - 1:
                    js_a[par, level] = combine(dot(tall(value), lift[level]))
                    copy_a = start(js_a.at[par, level], jr_a.at[par, level], 2**level)
                js_b[par, level] = value
                copies_b.append(start(js_b.at[par, level], jr_b.at[par, level], 2**level))
                yield
            far = None
            for level in range(1, bits):
                copies_b[level].wait_recv()
                term = across(level, jr_b[par, level], js_b[par, level])
                far = term if far is None else far + term
            jsib[par, 2, pl.ds(mine, half)] = far
            piece = jsib.at[par, 2, pl.ds(mine, half)]
            copy = start(piece, piece, 1)
            yield
            copies_b[0].wait_recv()
            copy.wait_recv()
            value = lanes_of([jsib[par, 2], jsib[par, 1], jsib[par, 0, :, :rank]])
            value = combine(dot(tall(value), enter[...]))
            field_a[...] = combine(dot_nt(leaf_a[...], tall(value[:, :rank])))
            field_b[...] = combine(dot_nt(leaf_b[...], tall(value[:, rank:])))
            yield

        steps = inner()
        next(steps)
        inside = combine(dot(tree[0], stack[0]))

        def residual(i):
            part = fold_cols(dot(bases[0, i, 0], wide(inside[i * rank : (i + 1) * rank])))
            r_ref[i] = b_ref[i] - fold_cols(dot(near[0, i], xw[i])) - part

        residual(0)
        next(steps)
        hook()
        for i in range(1, leaves):
            residual(i)
        for copy in copies_w:
            copy.wait_recv()
        value = jw_send[par, me]
        for e in range(1, group):
            value = value + jw_recv[par, e]
        far = None
        for level in range(bits, last - 1):
            jhigh[par, level] = combine(dot(tall(value), lift[level]))
            jhigh[par, levels + level] = value
            copy_a = start(jhigh.at[par, level], jgot.at[par, level], 2**level)
            copy_b = start(
                jhigh.at[par, levels + level], jgot.at[par, levels + 2 + level], 2**level
            )
            copy_a.wait_recv()
            copy_b.wait_recv()
            term = across(level, jgot[par, levels + 2 + level], value)
            far = term if far is None else far + term
            value = jhigh[par, level] + jgot[par, level]
        low, high = last - 1, last
        jhigh[par, high] = combine(dot(tall(value), lift[low]))
        jhigh[par, low] = value
        copies_top = [
            start(jhigh.at[par, src], jgot.at[par, dst], mask)
            for src, dst, mask in (
                (high, high + 1, 2**high + 2**low),
                (high, high, 2**high),
                (high, high + 2, 2**low),
                (low, low, 2**low),
            )
        ]
        for _ in range(bits - 2):
            next(steps)
        hook()
        copies_top[3].wait_recv()
        term = across(low, jgot[par, low], value)
        far = term if far is None else far + term
        for copy in copies_top[:3]:
            copy.wait_recv()
        own = jhigh[par, high] + jgot[par, high + 2]
        far = far + across(high, jgot[par, high] + jgot[par, high + 1], own)
        jplane[par, pl.ds(my_rows, cut)] = far
        copies_f = []
        for e in range(group - 1, 0, -1):
            piece = jplane.at[par, pl.ds(my_rows, cut)]
            copies_f.append(start(piece, piece, e))
        for _ in steps:
            pass
        for copy in copies_f:
            copy.wait_recv()
        flat = tall(jplane[par])
        alpha = field_a[...] + combine(dot_nt(fall_a[...], flat[:, :rank]))
        sums = None
        for i in range(leaves):
            out = r_ref[i] - fold_cols(dot(bases[0, i, 0], wide(alpha[i * rank : (i + 1) * rank])))
            low_out = out.astype(BF16)
            rb[i] = low_out
            stack[0, block(i)] = wide(dot(vt[1, i], low_out))
            square = jnp.sum((out * out).reshape(-1, 8, columns), axis=0)
            sums = square if sums is None else sums + square
        nrm[pl.ds(k, 1)] = jnp.sum(sums, axis=0, keepdims=True)
        pl.when(k == STEPS - 1)(start_norms)
        beta = field_b[...] + combine(dot_nt(fall_b[...], flat))
        beta = beta + combine(dot(tree[1], stack[0]))
        for i in range(leaves):
            far = beta[i * rank : (i + 1) * rank].astype(BF16)
            value = x_ref[i] + (dot(near[1, i], rb[i]) + dot(bases[1, i, 0], far))
            x_ref[i] = value
            xw[i] = wide(value)
        for copy in started:
            copy.wait_send()

    def norm_round(index, value):
        lo, hi = norm_rounds(levels)[index]
        nsend[index, pl.ds(0, STEPS)] = value
        for m in range(2 ** (hi - lo) - 1, 0, -1):
            pltpu.make_async_remote_copy(
                src_ref=nsend.at[index, pl.ds(0, STEPS)],
                dst_ref=nrecv.at[index, m, pl.ds(0, STEPS)],
                send_sem=nsend_sem.at[index],
                recv_sem=nrecv_sem.at[index],
                device_id=device(m << lo),
                device_id_type=pl.DeviceIdType.MESH,
            ).start()

    def start_norms():
        norm_round(0, nrm[pl.ds(0, STEPS)])

    def finish_norms():
        waits = []
        for index, (lo, hi) in enumerate(norm_rounds(levels)):
            if index:
                norm_round(index, value)
            count = 2 ** (hi - lo)
            every = nrecv.at[index, pl.ds(1, count - 1), pl.ds(0, STEPS)]
            pltpu.make_async_copy(every, every, nrecv_sem.at[index]).wait()
            waits.append(pltpu.make_async_copy(every, every, nsend_sem.at[index]))
            value = nsend[index, pl.ds(0, STEPS)]
            for m in range(1, count):
                value = value + nrecv[index, m, pl.ds(0, STEPS)]
        norm_ref[...] = value
        for copy in waits:
            copy.wait()

    setup_chain(1)
    setup_up(1)
    loads["res"].wait()

    def prepare():
        prepare_response()
        setup_tree(0)
        pl.semaphore_wait(barrier, len(partners))

    def first():
        send_response(0, None)
        send_factors()
        lift_response(0)
        setup_pairs(1)
        loads["near", 1].wait()

    def second():
        chain_step(0)
        setup_couplings(1)
        setup_down(1)

    def third():
        for level in range(1, bits):
            forward_factor(level)
        loads["top", 0].wait()
        setup_near()
        chain_step(1)

    def fourth():
        setup_base()
        setup_tree(1)

    def fifth():
        for level in range(bits, last):
            forward_factor(level)
        for level in range(2, bits):
            chain_step(level)
        setup_rise()

    def sixth():
        setup_enter()
        for level in range(bits, last):
            chain_step(level)

    def eighth():
        chain_step(last)
        setup_cross(bits, levels)
        for copy in pending:
            copy.wait_send()

    apply_first(prepare, [first, second, third, fourth, fifth])
    merged(0, [sixth, setup_fall, eighth])

    def step(k, carry):
        merged(k, [])
        return carry

    lax.fori_loop(1, STEPS, step, 0)
    finish_norms()


def body(right_sides, near_blocks, leaf_bases, local_factors, upper_factors, top_couplings):
    bits_leaf = lax.axis_size("leaf").bit_length() - 1
    bits_rows = lax.axis_size("rows").bit_length() - 1
    levels = bits_leaf + bits_rows
    leaves, size = near_blocks.shape[1], near_blocks.shape[2]
    rank = leaf_bases.shape[4]
    columns = right_sides.shape[1]
    half = columns // 2
    bits = group_bits(levels)
    group = 2**bits
    cut = columns // group
    copies = 2 * (group - 1) + 2 * bits + 2 * (levels - 2 - bits) + 4
    nodes = local_factors.shape[1]
    heights = upper_factors.shape[2]
    flat = leaves * rank
    pair = 2 * rank
    rounds = len(norm_rounds(levels))
    vmem = pltpu.VMEM
    dma = pltpu.SemaphoreType.DMA
    out, norms = pl.pallas_call(
        functools.partial(kernel, bits_leaf, bits_rows),
        out_shape=(
            vmem((leaves, size, columns), F32),
            vmem((STEPS, columns), F32),
        ),
        in_specs=[pl.BlockSpec(memory_space=pl.ANY)] * 6,
        out_specs=(pl.BlockSpec(memory_space=vmem), pl.BlockSpec(memory_space=vmem)),
        scratch_shapes=[
            vmem((leaves, size, columns), F32),
            vmem((leaves, size, columns), F32),
            vmem((2, leaves, size, size), BF16),
            vmem((2, leaves, 2, size, rank), BF16),
            vmem((2, nodes, 3, rank, rank), BF16),
            vmem((2, heights, 3, rank, rank), BF16),
            vmem((2, 2, rank, rank), BF16),
            vmem((2, leaves, rank, size), BF16),
            vmem((leaves - 1, rank, 2 * rank), BF16),
            vmem((levels, rank, 2 * rank), BF16),
            vmem((2 * rank, leaves * rank), BF16),
            vmem((2 * leaves * rank, rank), BF16),
            vmem((nodes - 1, rank, 2 * columns), BF16),
            vmem((nodes - 1, rank, columns), F32),
            vmem((8, columns), F32),
            vmem((group, cut, rank), F32),
            vmem((group, cut, rank), F32),
            vmem((2 * levels, cut, rank), F32),
            vmem((2 * levels + 1, cut, rank), F32),
            vmem((columns, rank), F32),
            vmem((bits, half, rank), F32),
            vmem((bits, half, rank), F32),
            vmem((bits, half, rank), F32),
            vmem((bits, half, rank), F32),
            vmem((3, rank, columns), F32),
            vmem((columns, rank), F32),
            vmem((levels - 1, rank, 3 * rank), F32),
            vmem((levels - 1, rank, 3 * rank), F32),
            vmem((levels, rank, rank), F32),
            vmem((levels, rank, rank), F32),
            vmem((levels, pair, pair), F32),
            vmem((levels, pair, pair), F32),
            vmem((levels, 3 * rank, pair), F32),
            vmem((flat, rank), F32),
            vmem((pair, flat), F32),
            vmem((rank, flat), F32),
            vmem((2, 2, flat, rank), F32),
            vmem((leaves, 3 * rank, size), BF16),
            vmem((flat, columns), F32),
            vmem((2, 2 * flat, flat), BF16),
            vmem((2, flat, 2 * columns), BF16),
            vmem((2 * pair, flat), BF16),
            vmem((pair, flat), BF16),
            vmem((4 * pair, flat), BF16),
            vmem((2 * pair, flat), BF16),
            vmem((levels, pair, 2 * pair), BF16),
            vmem((levels, 3 * rank, 2 * pair), BF16),
            vmem((5 * rank, 2 * pair), BF16),
            vmem((2 * flat, rank), BF16),
            vmem((2 * flat, pair), BF16),
            vmem((2 * flat, rank), BF16),
            vmem((2 * flat, rank), BF16),
            vmem((leaves, size, 2 * columns), BF16),
            vmem((leaves, size, columns), BF16),
            vmem((flat, columns), F32),
            vmem((flat, columns), F32),
            vmem((2, group, cut, pair), F32),
            vmem((2, group, cut, pair), F32),
            vmem((2, 2 * levels, cut, pair), F32),
            vmem((2, 2 * levels + 2, cut, pair), F32),
            vmem((2, columns, pair), F32),
            vmem((2, bits, half, pair), F32),
            vmem((2, bits, half, pair), F32),
            vmem((2, bits, half, pair), F32),
            vmem((2, bits, half, pair), F32),
            vmem((2, 3, columns, pair), F32),
            vmem((2, columns, pair), F32),
            vmem((rounds, 8, columns), F32),
            vmem((rounds, 32, 8, columns), F32),
            dma((12,)),
            dma((copies,)),
            dma((2, copies)),
            dma((3 * levels,)),
            dma((3 * levels,)),
            dma((rounds,)),
            dma((rounds,)),
        ],
        compiler_params=pltpu.CompilerParams(
            collective_id=0, has_side_effects=True, vmem_limit_bytes=60000000
        ),
    )(
        right_sides.reshape(leaves, size, columns),
        near_blocks,
        leaf_bases,
        local_factors,
        upper_factors,
        top_couplings,
    )
    return out.reshape(-1, columns), norms


def solution(mesh):
    placed = (
        P(("rows", "leaf"), None),
        P(None, ("rows", "leaf"), None, None),
        P(None, ("rows", "leaf"), None, None, None),
        P(None, ("rows", "leaf"), None, None, None),
        P(None, ("rows", "leaf"), None, None, None, None),
        P(),
    )
    return jax.shard_map(
        body,
        mesh=mesh,
        in_specs=placed,
        out_specs=(P(("rows", "leaf"), None), P()),
        check_vma=False,
    )
```
